32 devices in a mesh: dp: 8 (over y, x, core), mp: 4 (over z).
Axes of the slice: x: 2, y: 2, z: 4, core: 2. Of those that a mesh axis runs over, the one named last changes fastest.
Arguments:
- activations: bfloat16 [8192, 1280], P(('dp', 'mp')), may hold values from -6 to 6
- cotangent: bfloat16 [8192, 1280], P(('dp', 'mp')), may hold values from -6 to 6
- doc_lengths: int32 [8, 8], P('dp'), may hold values from 1 to 512, 1024 in all within a row
- w_in: float32 [4, 1280, 1280], P(None, 'dp', 'mp'), may hold values from -0.15625 to 0.15625
- w_attn_out: float32 [1280, 1280], P('mp', 'dp'), may hold values from -1.25 to 1.25
- w_down: float32 [1280, 1280], P('mp', 'dp'), may hold values from -0.15625 to 0.15625
- gains: float32 [2, 1280], replicated, may hold values from 0.5 to 1.5
- scale_param: float32 [80], replicated, may hold values from 0.5 to 2.5
- mom_in: float32 [4, 1280, 1280], P(None, 'dp', 'mp'), may hold values from -3 to 3
- mom_out: float32 [2, 1280, 1280], P(None, 'mp', 'dp'), may hold values from -3 to 3
- mom_gain: float32 [2, 1280], replicated, may hold values from -6 to 6
- mom_scale: float32 [80], replicated, may hold values from -6 to 6
- error_buffer: float32 [8, 6, 1280, 1280], P('dp', None, 'mp'), may hold values from -1.5 to 1.5
- factors: float32 [6, 1280, 8], P(None, 'mp'), may hold values from -6 to 6
Outputs:
- output: bfloat16 [8192, 1280], P(('dp', 'mp'))
- grad_input: float32 [8192, 1280], P(('dp', 'mp'))
- grad_in: float32 [4, 1280, 1280], P(None, 'dp', 'mp')
- grad_out: float32 [2, 1280, 1280], P(None, 'mp', 'dp')
- grad_gain: float32 [2, 1280], replicated
- grad_scale: float32 [80], replicated
- new_in: float32 [4, 1280, 1280], P(None, 'dp', 'mp')
- new_out: float32 [2, 1280, 1280], P(None, 'mp', 'dp')
- new_gain: float32 [2, 1280], replicated
- new_scale: float32 [80], replicated
- mom_in_new: float32 [4, 1280, 1280], P(None, 'dp', 'mp')
- mom_out_new: float32 [2, 1280, 1280], P(None, 'mp', 'dp')
- mom_gain_new: float32 [2, 1280], replicated
- mom_scale_new: float32 [80], replicated
- error_new: float32 [8, 6, 1280, 1280], P('dp', None, 'mp')
- factors_new: float32 [6, 1280, 8], P(None, 'mp')
The draws below stay inside these ranges and needn't reach their ends.
Inputs may be any that keep to these rules, and one draw needn't show every extreme that they name: `doc_lengths`: each row gives 8 document lengths that fill one sequence of 1024 tokens; in each row the longest is exactly 512.
All inputs are finite; a program needn't handle non-finite values.
Results may differ from the reference program's by a relative error of at most 0.014.
The reference program's roundings to bfloat16 on the way count: a program that leaves them out, or rounds other values in their place, can miss the bound.
Values may be sent and summed in bfloat16 or wider, within the bound.
A program may use at most 192 MiB of HBM per device.

```python
import math
from functools import partial
import jax
import jax.numpy as jnp
import numpy as np
from jax import lax

D = 1280
FF = 1280
HEADS = 16
HD = 80
NDOC = 8
RANK = 8
SEQ = 1024
NSEQ = 8
LMAX = 512
TOKENS = 8192


def block_scale(key, extent, shards, least, top_value):
    loudness, own = 1.0, jax.random.fold_in(key, 6)
    for dim, blocks in shards:
        steps = jnp.exp(jax.random.uniform(jax.random.fold_in(own, dim), (blocks,), jnp.float32, least / len(shards), top_value / len(shards)))
        loudness = loudness * jnp.repeat(steps, extent[dim] // blocks).reshape([-1 if axis == dim else 1 for axis in range(len(extent))])
    return loudness


def profile(amount, total, reach, slope):
    weights = [(1 << 20) // math.isqrt(grade ** slope) + 1 for grade in range(2, amount + 1)]
    spare, given = total - reach - (amount - 1), [1] * (amount - 1)
    while spare > 0:
        movable = [i for i in range(amount - 1) if given[i] < reach]
        mass, remaining = sum([weights[i] for i in movable]), spare
        for i in movable:
            extra = min(reach - given[i], max(1, remaining * weights[i] // mass), spare)
            given[i] = given[i] + extra
            spare = spare - extra
    return np.array([reach] + given)


def uneven(stream_key, number_of, total, most, skew):
    if number_of == 2:
        one = jax.random.randint(stream_key, (), max(1, total - most), min(most, total - 1) + 1)
        return jnp.stack([one, total - one])
    sizes = jnp.asarray(profile(number_of, total, most, skew), jnp.int32)
    couples = (number_of - 1) // 2
    giver, taker = sizes[1:1 + 2 * couples:2], sizes[2:2 + 2 * couples:2]
    room = jnp.minimum(giver - 1, most - taker)
    shifted = jax.random.randint(jax.random.fold_in(stream_key, 1), (couples,), 0, 1 << 20) % (room + 1)
    sizes = sizes.at[1:1 + 2 * couples:2].set(giver - shifted).at[2:2 + 2 * couples:2].set(taker + shifted)
    return sizes[jax.random.permutation(jax.random.fold_in(stream_key, 2), number_of)]


def bell_draw(stream_key, shape, width, most, shards=(), kind=jnp.bfloat16):
    values = jax.random.normal(stream_key, shape, jnp.float32) * width
    if len(shards) > 0:
        values = block_scale(stream_key, shape, shards, -0.22, 0.18) * values
    return jnp.clip(values, min=-most, max=most).astype(kind)


def setup_inputs(seed: int = 0) -> dict:
    key_list = jax.random.split(jax.random.key(seed), 15)
    activations = bell_draw(key_list[0], (TOKENS, D), 1.0, 6.0, ((0, 32),))
    cotangent = bell_draw(key_list[1], (TOKENS, D), 1.0, 6.0, ((0, 32),))
    doc_lengths = jax.vmap(lambda own: uneven(own, NDOC, SEQ, LMAX, 2))(jax.random.split(key_list[2], NSEQ)).reshape((NSEQ, NDOC)).astype(jnp.int32)
    w_in = bell_draw(key_list[3], (4, D, D), D ** -0.5, 0.15625, ((1, 8), (2, 4)), jnp.float32)
    w_attn_out = bell_draw(key_list[4], (D, D), (D // 64) ** -0.5, 1.25, ((0, 4), (1, 8)), jnp.float32)
    w_down = bell_draw(key_list[5], (FF, D), FF ** -0.5, 0.15625, ((0, 4), (1, 8)), jnp.float32)
    gains = jnp.clip(1.0 + 0.1 * jax.random.normal(key_list[6], (2, D), jnp.float32), 0.5, 1.5)
    scale_param = jnp.clip(jax.random.uniform(key_list[7], (HD,), jnp.float32, 0.5, 2.5), 0.5, 2.5)
    mom_in = bell_draw(key_list[8], (4, D, D), 0.2, 3.0, ((1, 8), (2, 4)), jnp.float32)
    mom_out = bell_draw(key_list[9], (2, D, D), 0.2, 3.0, ((1, 4), (2, 8)), jnp.float32)
    mom_gain = bell_draw(key_list[10], (2, D), 1.0, 6.0, (), jnp.float32)
    mom_scale = bell_draw(key_list[11], (HD,), 1.0, 6.0, (), jnp.float32)
    error_buffer = bell_draw(key_list[12], (NSEQ, 6, D, D), 0.1, 1.5, ((0, 8), (2, 4)), jnp.float32)
    factors = bell_draw(key_list[13], (6, D, RANK), 1.0, 6.0, ((1, 4),), jnp.float32)
    return dict(activations=activations, cotangent=cotangent, doc_lengths=doc_lengths, w_in=w_in, w_attn_out=w_attn_out, w_down=w_down, gains=gains, scale_param=scale_param, mom_in=mom_in, mom_out=mom_out, mom_gain=mom_gain, mom_scale=mom_scale, error_buffer=error_buffer, factors=factors)


HIGHEST = lax.Precision.HIGHEST
EPSILON = 1e-06
SCALE_BASE = 1.442695041
MOMENTUM = 0.9
RATE = 0.1
MASKED_SCORE = -1e+30

@jax.custom_vjp
def low(v):
    return lax.optimization_barrier(v.astype(jnp.bfloat16)).astype(jnp.float32)

@jax.custom_vjp
def low_back(v):
    return v

def low_keep(v):
    return (low(v), None)

def low_pass(kept, grad):
    return (grad,)

def back_keep(v):
    return (v, None)

def back_low(kept, grad):
    return (low(grad),)
low.defvjp(low_keep, low_pass)
low_back.defvjp(back_keep, back_low)

def segment_ids(lengths, count):
    ends = jnp.cumsum(lengths).astype(jnp.int32)
    position = jnp.arange(count, dtype=jnp.int32)
    return lax.optimization_barrier(jnp.sum((position[:, None] >= ends[None, :]).astype(jnp.int32), axis=1)).astype(jnp.int32)

def rms_scale(values):
    return lax.rsqrt(lax.optimization_barrier(jnp.mean(values * values, axis=-1, keepdims=True)) + EPSILON)

def orthonormal(matrix):
    columns = []
    for index in range(matrix.shape[-1]):
        vector = matrix[..., index]
        for basis in columns:
            vector = vector - lax.optimization_barrier(jnp.sum(basis * vector, axis=-1, keepdims=True)) * basis
        vector = vector * lax.rsqrt(lax.optimization_barrier(jnp.sum(vector * vector, axis=-1, keepdims=True)) + 1e-12)
        columns.append(vector)
    return jnp.stack(columns, axis=-1)

def attend_block(query, start, keys, values, segments):
    rows = query.shape[1]
    scores = low_back(jnp.einsum('hqd,hkd->hqk', query, keys, precision=HIGHEST))
    query_pos = start + jnp.arange(rows, dtype=jnp.int32)
    key_pos = jnp.arange(keys.shape[1], dtype=jnp.int32)
    query_seg = lax.dynamic_slice_in_dim(segments, start, rows)
    allowed = (key_pos[None, :] <= query_pos[:, None]) & (segments[None, :] == query_seg[:, None])
    masked = jnp.where(allowed[None], scores, MASKED_SCORE)
    highest = lax.optimization_barrier(jnp.max(masked, axis=-1, keepdims=True))
    raised = jnp.exp(masked - highest)
    probability = low(raised / lax.optimization_barrier(jnp.sum(raised, axis=-1, keepdims=True)))
    return jnp.einsum('hqk,hkd->hqd', probability, values, precision=HIGHEST)

def forward_sequence(inputs, w_in, w_attn_out, w_down, gains, scale_param, segments):
    count = inputs.shape[0]
    normed = low(inputs * rms_scale(inputs) * gains[0])
    query_raw = low_back(jnp.dot(normed, low(w_in[0]), precision=HIGHEST))
    factor = SCALE_BASE / math.sqrt(HD) * jax.nn.softplus(scale_param)
    query = low(query_raw * jnp.tile(factor, HEADS))
    keys = low(low_back(jnp.dot(normed, low(w_in[1]), precision=HIGHEST)))
    values = low(low_back(jnp.dot(normed, low(w_in[2]), precision=HIGHEST)))

    def to_heads(table):
        return table.reshape(count, HEADS, HD).transpose(1, 0, 2)
    block = min(512, count)
    block_count = count // block
    query_blocks = to_heads(query).reshape(HEADS, block_count, block, HD).transpose(1, 0, 2, 3)
    starts = jnp.arange(block_count, dtype=jnp.int32) * block
    checked = jax.checkpoint(attend_block)
    key_heads = to_heads(keys)
    value_heads = to_heads(values)
    outcome = lax.map(lambda item: checked(item[0], item[1], key_heads, value_heads, segments), (query_blocks, starts))
    attended = outcome.transpose(1, 0, 2, 3).reshape(HEADS, count, HD).transpose(1, 0, 2).reshape(count, HEADS * HD)
    attended = low(low_back(attended))
    branch = low_back(jnp.dot(attended, low(w_attn_out), precision=HIGHEST))
    middle = inputs + branch
    normed_two = low(middle * rms_scale(middle) * gains[1])
    gate = low_back(jnp.dot(normed_two, low(w_in[3]), precision=HIGHEST))
    hidden = low(jax.nn.silu(gate))
    return middle + low_back(jnp.dot(hidden, low(w_down), precision=HIGHEST))

def reference(activations, cotangent, doc_lengths, w_in, w_attn_out, w_down, gains, scale_param, mom_in, mom_out, mom_gain, mom_scale, error_buffer, factors):
    inputs = activations.astype(jnp.float32).reshape(NSEQ, SEQ, D)
    grads_out = cotangent.astype(jnp.float32).reshape(NSEQ, SEQ, D)

    def per_sequence(carry, item):
        seq_inputs, seq_grads, lengths = item
        segments = segment_ids(lengths, SEQ)
        result, pullback = jax.vjp(partial(forward_sequence, segments=segments), seq_inputs, w_in, w_attn_out, w_down, gains, scale_param)
        return (carry, (result,) + tuple(pullback(seq_grads)))
    carry, stacked = lax.scan(per_sequence, jnp.zeros((), jnp.float32), (inputs, grads_out, doc_lengths))
    result, grad_x, g_in, g_attn, g_down, g_gains, g_scale = stacked
    scaling = TOKENS ** (-0.5)
    grad_in = scaling * lax.optimization_barrier(jnp.sum(g_in, axis=0))
    grad_out = scaling * jnp.stack([lax.optimization_barrier(jnp.sum(g_attn, axis=0)), lax.optimization_barrier(jnp.sum(g_down, axis=0))])
    grad_gain = scaling * lax.optimization_barrier(jnp.sum(g_gains, axis=0))
    grad_scale = scaling * lax.optimization_barrier(jnp.sum(g_scale, axis=0))
    matrices = scaling * jnp.concatenate([g_in, jnp.swapaxes(g_attn, 1, 2)[:, None], jnp.swapaxes(g_down, 1, 2)[:, None]], axis=1) + jnp.swapaxes(error_buffer, 2, 3)
    left = jnp.einsum('skdc,kcr->kdr', matrices, factors, precision=HIGHEST)
    basis = orthonormal(left)
    right = jnp.einsum('skdc,kdr->kcr', matrices, basis, precision=HIGHEST)
    approx = jnp.einsum('kdr,kcr->kdc', basis, right, precision=HIGHEST)
    error_new = jnp.swapaxes(matrices - approx[None], 2, 3)
    mom_in_new = MOMENTUM * mom_in + approx[:4]
    new_in = w_in - RATE * mom_in_new
    mom_out_new = MOMENTUM * mom_out + jnp.swapaxes(approx[4:], 1, 2)
    new_out = jnp.stack([w_attn_out, w_down]) - RATE * mom_out_new
    mom_gain_new = MOMENTUM * mom_gain + grad_gain
    new_gain = gains - RATE * mom_gain_new
    mom_scale_new = MOMENTUM * mom_scale + grad_scale
    new_scale = scale_param - RATE * mom_scale_new
    return (result.reshape(TOKENS, D).astype(jnp.bfloat16), grad_x.reshape(TOKENS, D), grad_in, grad_out, grad_gain, grad_scale, new_in, new_out, new_gain, new_scale, mom_in_new, mom_out_new, mom_gain_new, mom_scale_new, error_new, right)
```

```python
import functools
import math

import jax
import jax.numpy as jnp
from jax import lax
from jax.experimental import pallas as pl
from jax.experimental.pallas import tpu as pltpu
from jax.sharding import PartitionSpec as P

HD = 80
LANE = 128
HIGHEST = lax.Precision.HIGHEST
EPSILON = 1e-06
SCALE_BASE = 1.442695041
MOMENTUM = 0.9
RATE = 0.1
NEG = -1e30
F32 = jnp.float32
BF16 = jnp.bfloat16
MESH = pl.DeviceIdType.MESH
VMEM_LIMIT = 62 * 1024 * 1024


def nn(a, b):
    return jnp.dot(a, b, preferred_element_type=F32)


def nt(a, b):
    return lax.dot_general(a, b, (((1,), (1,)), ((), ())), preferred_element_type=F32)


def tn(a, b):
    return lax.dot_general(a, b, (((0,), (0,)), ((), ())), preferred_element_type=F32)


def spread(cols, heads):
    row = lax.broadcasted_iota(jnp.int32, (cols, heads * LANE), 0)
    col = lax.broadcasted_iota(jnp.int32, (cols, heads * LANE), 1)
    off = col & (LANE - 1)
    hit = (row == (col >> 7) * HD + off) & (off < HD)
    return jnp.where(hit, 1.0, 0.0).astype(BF16)


def block_rows(index, rows):
    return pl.ds(pl.multiple_of(index * rows, rows), rows)


def greet(peers):
    bar = pltpu.get_barrier_semaphore()
    for peer in peers:
        pl.semaphore_signal(bar, 1, device_id=peer, device_id_type=MESH)
    pl.semaphore_wait(bar, len(peers))


def line_peers(n, me):
    return [{"mp": lax.rem(me + off, n)} for off in range(1, n)]


class LineGather:
    def __init__(self, n, me, own, buf, ssem, rsem):
        self.n, self.me, self.own, self.buf = n, me, own, buf
        self.ssem, self.rsem = ssem, rsem

    def copy(self, slot, hop, way):
        src = self.own if hop == 0 else self.buf.at[slot]
        return pltpu.make_async_remote_copy(
            src_ref=src,
            dst_ref=self.buf.at[slot],
            send_sem=self.ssem.at[way, hop],
            recv_sem=self.rsem.at[slot],
            device_id={"mp": self.me + 1 - 2 * way},
            device_id_type=MESH,
        )

    def goes(self, hop, way):
        if way == 0:
            return (self.me - hop >= 0) & (self.me < self.n - 1)
        return (self.me + hop <= self.n - 1) & (self.me > 0)

    def slot(self, hop, way):
        return self.me - hop if way == 0 else self.me + hop

    def arrives(self, hop, way):
        return self.me - hop >= 0 if way == 0 else self.me + hop <= self.n - 1

    def send(self, hop, ways=(0, 1)):
        for way in ways:

            @pl.when(self.goes(hop, way))
            def _(way=way):
                self.copy(self.slot(hop, way), hop, way).start()

    def relay(self, hop):
        for way in (0, 1):

            @pl.when(self.arrives(hop, way))
            def _(way=way):
                slot = self.slot(hop, way)
                self.copy(slot, hop, way).wait_recv()

            if hop < self.n - 1:
                self.send(hop, (way,))

    def finish(self):
        for hop in range(self.n - 1):
            for way in (0, 1):

                @pl.when(self.goes(hop, way))
                def _(way=way, hop=hop):
                    self.copy(self.slot(hop, way), hop, way).wait_send()


def line_sems(n):
    return [pltpu.SemaphoreType.DMA((2, n)), pltpu.SemaphoreType.DMA((n,))]


def vmem(count):
    return [pl.BlockSpec(memory_space=pltpu.VMEM)] * count


def params(collective_id=None):
    return pltpu.CompilerParams(
        collective_id=collective_id,
        has_side_effects=collective_id is not None,
        vmem_limit_bytes=VMEM_LIMIT,
    )


def attend_kernel(
    dims, x_ref, w_ref, gain_ref, c_ref, st_ref,
    n1_ref, q_ref, k_ref, v_ref, lse_ref, oc_ref, of_ref,
    xbuf, wpad, mask, opad, zs, zr, as_, ar,
):
    n, rows, heads, span = dims
    me = lax.axis_index("mp")
    cols = w_ref.shape[2]
    greet(line_peers(n, me))
    gather = LineGather(n, me, x_ref, xbuf, zs, zr)
    gather.send(0)
    sel = spread(cols, heads)
    for m in range(3):
        wpad[m] = nn(w_ref[m], sel).astype(BF16)
    xbuf[me] = x_ref[...]

    def project(slot):
        x = xbuf[slot].astype(F32)
        scale = lax.rsqrt(jnp.mean(x * x, axis=-1, keepdims=True) + EPSILON)
        normed = (x * scale * gain_ref[...]).astype(BF16)
        n1_ref[slot] = normed
        at = block_rows(slot, rows)
        for m, ref in enumerate((q_ref, k_ref, v_ref)):
            out = nn(normed, wpad[m])
            if m == 0:
                out = out * c_ref[...]
            out = out.astype(BF16)
            for h in range(heads):
                ref[h, at, :] = out[:, h * LANE : (h + 1) * LANE]

    project(me)

    def arrivals(hop):
        def one(way, _):
            slot = me - hop + 2 * hop * way

            @pl.when((slot >= 0) & (slot < n))
            def _():
                project(slot)

            return 0

        lax.fori_loop(0, 2, one, 0)

    for hop in range(1, n):
        gather.relay(hop)
        arrivals(hop)

    def chunk(i, _):
        first = jnp.maximum(i - (span - 1), 0)
        at, keys = block_rows(i, rows), pl.ds(pl.multiple_of(first * rows, rows), span * rows)
        q_pos = i * rows + lax.broadcasted_iota(jnp.int32, mask.shape, 0)
        k_pos = first * rows + lax.broadcasted_iota(jnp.int32, mask.shape, 1)
        mask[...] = jnp.where((k_pos <= q_pos) & (k_pos >= st_ref[at, :]), 0.0, NEG)

        def head(h, _):
            scores = nt(q_ref[h, at, :], k_ref[h, keys, :]) + mask[...]
            top = jnp.max(scores, axis=-1, keepdims=True)
            raised = jnp.exp(scores - top)
            total = jnp.sum(raised, axis=-1, keepdims=True)
            prob = (raised * (1.0 / total)).astype(BF16)
            opad[h] = nn(prob, v_ref[h, keys, :]).astype(BF16)
            lse_ref[h, at, :] = top + jnp.log(total)
            return 0

        lax.fori_loop(0, heads, head, 0)
        wide = jnp.concatenate([opad[h] for h in range(heads)], axis=1)
        oc_ref[i] = nt(wide, sel).astype(BF16)

        @pl.when(i != me)
        def _():
            pltpu.make_async_remote_copy(
                src_ref=oc_ref.at[i], dst_ref=of_ref.at[me], send_sem=as_.at[i],
                recv_sem=ar.at[me], device_id={"mp": i}, device_id_type=MESH,
            ).start()

        @pl.when(i == me)
        def _():
            of_ref[me] = oc_ref[me]

        return 0

    lax.fori_loop(0, n, chunk, 0)
    gather.finish()
    for off in range(1, n):
        peer = lax.rem(me + off, n)
        copy = pltpu.make_async_remote_copy(
            src_ref=oc_ref.at[peer], dst_ref=of_ref.at[peer], send_sem=as_.at[peer],
            recv_sem=ar.at[peer], device_id={"mp": peer}, device_id_type=MESH,
        )
        copy.wait_send()
        copy.wait_recv()


def attend(dims, x, w, gain, c_row, starts):
    n, rows, heads, span = dims
    width, cols = x.shape[1], w.shape[2]
    count = n * rows
    head_out = jax.ShapeDtypeStruct((heads, count, LANE), BF16)
    return pl.pallas_call(
        functools.partial(attend_kernel, dims),
        out_shape=(
            jax.ShapeDtypeStruct((n, rows, width), BF16),
            head_out, head_out, head_out,
            jax.ShapeDtypeStruct((heads, count, 1), F32),
            jax.ShapeDtypeStruct((n, rows, cols), BF16),
            jax.ShapeDtypeStruct((n, rows, cols), BF16),
        ),
        in_specs=vmem(5),
        out_specs=vmem(7),
        scratch_shapes=[
            pltpu.VMEM((n, rows, width), BF16),
            pltpu.VMEM((3, width, heads * LANE), BF16),
            pltpu.VMEM((rows, span * rows), F32),
            pltpu.VMEM((heads, rows, LANE), BF16),
            *line_sems(n),
            pltpu.SemaphoreType.DMA((n,)),
            pltpu.SemaphoreType.DMA((n,)),
        ],
        compiler_params=params(1),
        name="attend",
    )(x, w, gain, c_row, starts)


def middle_kernel(
    dims, x_ref, g_ref, of_ref, w_ref, gain_ref,
    out_ref, dh_ref, n2_ref, g_all, dhb_ref, dgain_ref,
    h_ref, acc, dn2, gs, gr, ns, nr, ds, dr,
):
    n = dims[0]
    me = lax.axis_index("mp")
    greet(line_peers(n, me))
    gather_g = LineGather(n, me, g_ref, g_all, gs, gr)
    gather_n = LineGather(n, me, n2_ref.at[me], n2_ref, ns, nr)
    gather_d = LineGather(n, me, dhb_ref.at[me], dhb_ref, ds, dr)
    gather_g.send(0)
    g_all[me] = g_ref[...]
    h_ref[...] = x_ref[...].astype(F32)

    def project(j, _):
        h_ref[...] += nt(of_ref[j], w_ref[j, 0])
        return 0

    lax.fori_loop(0, n, project, 0)
    h = h_ref[...]
    scale = lax.rsqrt(jnp.mean(h * h, axis=-1, keepdims=True) + EPSILON)
    n2_ref[me] = (h * scale * gain_ref[...]).astype(BF16)
    gather_n.send(0)
    acc[...] = h_ref[...]
    dn2[...] = jnp.zeros_like(dn2)

    def hidden(j, _):
        gate = nn(n2_ref[me], w_ref[j, 1])
        sig = 1.0 / (1.0 + jnp.exp(-gate))
        acc[...] += nt((gate * sig).astype(BF16), w_ref[j, 2])
        dz = nn(g_ref[...], w_ref[j, 2])
        da = (dz * (sig * (1.0 + gate * (1.0 - sig)))).astype(BF16)
        dn2[...] += nt(da, w_ref[j, 1])
        return 0

    lax.fori_loop(0, n, hidden, 0)
    out_ref[...] = acc[...].astype(BF16)
    h = h_ref[...]
    scale = lax.rsqrt(jnp.mean(h * h, axis=-1, keepdims=True) + EPSILON)
    unit = h * scale
    grad = dn2[...]
    dgain_ref[...] = jnp.sum(grad * unit, axis=0, keepdims=True)
    du = grad * gain_ref[...]
    dh = g_ref[...].astype(F32) + scale * (du - unit * jnp.mean(du * unit, axis=-1, keepdims=True))
    dh_ref[...] = dh
    dhb_ref[me] = dh.astype(BF16)
    gather_d.send(0)
    for hop in range(1, n):
        gather_g.relay(hop)
        gather_n.relay(hop)
        gather_d.relay(hop)
    for gather in (gather_g, gather_n, gather_d):
        gather.finish()


def middle(dims, x, g, o_full, w_full, gain):
    n, rows = dims[:2]
    width = x.shape[1]
    every = jax.ShapeDtypeStruct((n, rows, width), BF16)
    return pl.pallas_call(
        functools.partial(middle_kernel, dims),
        out_shape=(
            jax.ShapeDtypeStruct((rows, width), BF16),
            jax.ShapeDtypeStruct((rows, width), F32),
            every, every, every,
            jax.ShapeDtypeStruct((1, width), F32),
        ),
        in_specs=vmem(5),
        out_specs=vmem(6),
        scratch_shapes=[pltpu.VMEM((rows, width), F32)] * 3 + line_sems(n) * 3,
        compiler_params=params(2),
        name="middle",
    )(x, g, o_full, w_full, gain)


def back_kernel(
    dims, q_ref, k_ref, v_ref, lse_ref, dhb_ref, w_ref, c_ref, st_ref,
    dx_ref, dc_ref,
    wpad, mask, do_ref, dq_ref, dk_ref, dv_ref,
):
    n, rows, heads, span = dims
    sel = spread(w_ref.shape[1], heads)
    wpad[...] = nn(w_ref[...], sel).astype(BF16)
    dk_ref[...] = jnp.zeros_like(dk_ref)
    dv_ref[...] = jnp.zeros_like(dv_ref)
    dc_ref[...] = jnp.zeros_like(dc_ref)

    def squeeze(ref, at):
        wide = jnp.concatenate([ref[h, at, :].astype(BF16) for h in range(heads)], axis=1)
        return nt(wide, sel).astype(BF16)

    def chunk(i, _):
        first = jnp.maximum(i - (span - 1), 0)
        at, keys = block_rows(i, rows), pl.ds(pl.multiple_of(first * rows, rows), span * rows)
        q_pos = i * rows + lax.broadcasted_iota(jnp.int32, mask.shape, 0)
        k_pos = first * rows + lax.broadcasted_iota(jnp.int32, mask.shape, 1)
        mask[...] = jnp.where((k_pos <= q_pos) & (k_pos >= st_ref[at, :]), 0.0, NEG)
        grad = nn(dhb_ref[i], wpad[...]).astype(BF16)
        for h in range(heads):
            do_ref[h] = grad[:, h * LANE : (h + 1) * LANE]

        def head(h, _):
            query = q_ref[h, at, :]
            scores = nt(query, k_ref[h, keys, :]) + mask[...]
            prob = jnp.exp(scores - lse_ref[h, at, :])
            dp = nt(do_ref[h], v_ref[h, keys, :])
            inner = jnp.sum(prob * dp, axis=-1, keepdims=True)
            ds = (prob * (dp - inner)).astype(BF16)
            dq = nn(ds, k_ref[h, keys, :])
            dk_ref[h, keys, :] += tn(ds, query)
            dv_ref[h, keys, :] += tn(prob.astype(BF16), do_ref[h])
            dc_ref[...] += jnp.sum(dq * query.astype(F32), axis=0, keepdims=True)
            dq_ref[h] = (dq * c_ref[:, :LANE]).astype(BF16)
            return 0

        lax.fori_loop(0, heads, head, 0)
        dx_ref[0, i] = squeeze(dq_ref, slice(None))
        return 0

    lax.fori_loop(0, n, chunk, 0)

    def close(i, _):
        at = block_rows(i, rows)
        dx_ref[1, i] = squeeze(dk_ref, at)
        dx_ref[2, i] = squeeze(dv_ref, at)
        return 0

    lax.fori_loop(0, n, close, 0)


def back(dims, q, k, v, lse, dhb, w_out, c_row, starts):
    n, rows, heads, span = dims
    cols, width = w_out.shape[1], w_out.shape[0]
    return pl.pallas_call(
        functools.partial(back_kernel, dims),
        out_shape=(
            jax.ShapeDtypeStruct((3, n, rows, cols), BF16),
            jax.ShapeDtypeStruct((1, LANE), F32),
        ),
        in_specs=vmem(8),
        out_specs=vmem(2),
        scratch_shapes=[
            pltpu.VMEM((width, heads * LANE), BF16),
            pltpu.VMEM((rows, span * rows), F32),
            pltpu.VMEM((heads, rows, LANE), BF16),
            pltpu.VMEM((heads, rows, LANE), BF16),
            pltpu.VMEM((heads, n * rows, LANE), F32),
            pltpu.VMEM((heads, n * rows, LANE), F32),
        ],
        compiler_params=params(),
        name="back",
    )(q, k, v, lse, dhb, w_out, c_row, starts)


def grads_kernel(
    dims, n1_ref, n2_ref, dhb_ref, g_ref, dx_ref, oc_ref, wqkv_ref, wup_ref, wdn_ref,
    x_ref, dh_ref, gain_ref,
    gt_ref, gb_ref, gin_ref, dgain_ref,
    z_ref, da_ref, sbuf, lbuf, rbuf, ss, ls, rs,
):
    n, rows, heads, span = dims
    me = lax.axis_index("mp")
    greet(line_peers(n, me))

    def own(i):
        total = nt(dx_ref[0, i], wqkv_ref[0])
        total += nt(dx_ref[1, i], wqkv_ref[1])
        return total + nt(dx_ref[2, i], wqkv_ref[2])

    def copy(i, way):
        buf, sem = (lbuf, ls) if way == 0 else (rbuf, rs)
        return pltpu.make_async_remote_copy(
            src_ref=sbuf.at[i], dst_ref=buf.at[i], send_sem=ss.at[i], recv_sem=sem.at[i],
            device_id={"mp": me + 1 - 2 * way}, device_id_type=MESH,
        )

    def step(t, way):
        i = n - 1 - t if way == 0 else t
        buf = lbuf if way == 0 else rbuf
        has = me > 0 if way == 0 else me < n - 1

        @pl.when(i > me if way == 0 else i < me)
        def _():
            mine = own(i)

            @pl.when(has)
            def _():
                copy(i, way).wait_recv()
                sbuf[i] = (mine + buf[i].astype(F32)).astype(BF16)

            @pl.when(jnp.logical_not(has))
            def _():
                sbuf[i] = mine.astype(BF16)

            copy(i, way).start()

    def hidden(i, _):
        gate = nn(n2_ref[i], wup_ref[...])
        sig = 1.0 / (1.0 + jnp.exp(-gate))
        z_ref[i] = (gate * sig).astype(BF16)
        dz = nn(g_ref[i], wdn_ref[...])
        da_ref[i] = (dz * (sig * (1.0 + gate * (1.0 - sig)))).astype(BF16)
        return 0

    def flat(value):
        return value.reshape(n * rows, value.shape[-1])

    def weight(m, a, b):
        left, right = flat(a), flat(b)
        gt_ref[m] = tn(right, left)
        gb_ref[m] = tn(left, right).astype(BF16)

    step(0, 0)
    step(0, 1)
    lax.fori_loop(0, n, hidden, 0)
    weight(3, n2_ref[...], da_ref[...])
    weight(5, g_ref[...], z_ref[...])
    weight(4, dhb_ref[...], oc_ref[...])
    for t in range(1, n - 1):
        step(t, 0)
        step(t, 1)

    def inputs(m, _):
        weight(m, n1_ref[...], dx_ref[m])
        return 0

    lax.fori_loop(0, 3, inputs, 0)
    gin_ref[...] = own(me)

    @pl.when(me > 0)
    def _():
        copy(me, 0).wait_recv()
        gin_ref[...] += lbuf[me].astype(F32)

    @pl.when(me < n - 1)
    def _():
        copy(me, 1).wait_recv()
        gin_ref[...] += rbuf[me].astype(F32)

    x = x_ref[...].astype(F32)
    scale = lax.rsqrt(jnp.mean(x * x, axis=-1, keepdims=True) + EPSILON)
    unit = x * scale
    grad = gin_ref[...]
    dgain_ref[...] = jnp.sum(grad * unit, axis=0, keepdims=True)
    du = grad * gain_ref[...]
    gin_ref[...] = dh_ref[...] + scale * (du - unit * jnp.mean(du * unit, axis=-1, keepdims=True))
    for i in range(n):

        @pl.when(me < i)
        def _(i=i):
            copy(i, 0).wait_send()

        @pl.when(me > i)
        def _(i=i):
            copy(i, 1).wait_send()


def grads(dims, n1, n2, dhb, g_all, dx, oc, wqkv, w_up, w_down, x, dh, gain):
    n, rows = dims[:2]
    width, cols = w_up.shape
    every = pltpu.VMEM((n, rows, width), BF16)
    return pl.pallas_call(
        functools.partial(grads_kernel, dims),
        out_shape=(
            jax.ShapeDtypeStruct((6, cols, width), F32),
            jax.ShapeDtypeStruct((6, width, cols), BF16),
            jax.ShapeDtypeStruct((rows, width), F32),
            jax.ShapeDtypeStruct((1, width), F32),
        ),
        in_specs=vmem(12),
        out_specs=vmem(4),
        scratch_shapes=[
            pltpu.VMEM((n, rows, cols), BF16),
            pltpu.VMEM((n, rows, cols), BF16),
            every, every, every,
            pltpu.SemaphoreType.DMA((n,)),
            pltpu.SemaphoreType.DMA((n,)),
            pltpu.SemaphoreType.DMA((n,)),
        ],
        compiler_params=params(3),
        name="grads",
    )(n1, n2, dhb, g_all, dx, oc, wqkv, w_up, w_down, x, dh, gain)


def orthonormal(matrix):
    columns = []
    for index in range(matrix.shape[-1]):
        vector = matrix[..., index]
        for basis in columns:
            vector = vector - jnp.sum(basis * vector, axis=-1, keepdims=True) * basis
        vector = vector * lax.rsqrt(jnp.sum(vector * vector, axis=-1, keepdims=True) + 1e-12)
        columns.append(vector)
    return jnp.stack(columns, axis=-1)


def on_device(
    activations, cotangent, doc_lengths, w_in, w_attn_out, w_down, gains, scale_param,
    mom_in, mom_out, mom_gain, mom_scale, error_buffer, factors,
):
    rows, width = activations.shape
    n = lax.axis_size("mp")
    data_par = lax.axis_size("dp")
    my_data, me = lax.axis_index("dp"), lax.axis_index("mp")
    count = rows * n
    scaling = (count * data_par) ** (-0.5)
    cols = w_in.shape[2]
    own_rows = w_in.shape[1]
    heads = cols // HD
    longest = count // 2
    span = min(n, -(-(longest - 1) // rows) + 1)
    dims = (n, rows, heads, span)

    shards = jnp.concatenate([w_in, w_attn_out.T[None], w_down.T[None]], axis=0).astype(BF16)
    wqkv = lax.all_gather(shards[:3], "dp", axis=1, tiled=True)
    tail = jnp.stack([shards[4], shards[3], shards[5]])
    w_full = lax.all_gather(lax.all_gather(tail, "mp", axis=0), "dp", axis=2, tiled=True)
    w_mine = lax.dynamic_index_in_dim(w_full, me, 0, keepdims=False)

    ends = jnp.cumsum(doc_lengths[0])
    position = jnp.arange(count, dtype=jnp.int32)[:, None]
    starts = jnp.max(jnp.where(ends[None, :] <= position, ends[None, :], 0), axis=1, keepdims=True)
    factor = SCALE_BASE / math.sqrt(HD) * jax.nn.softplus(scale_param)
    c_row = jnp.tile(jnp.pad(factor, (0, LANE - HD)), heads)[None]

    n1, q, k, v, lse, oc, o_full = attend(dims, activations, wqkv, gains[:1], c_row, starts)
    output, dh, n2, g_all, dhb, dgain2 = middle(dims, activations, cotangent, o_full, w_full, gains[1:])
    dx, dc = back(dims, q, k, v, lse, dhb, w_mine[0], c_row, starts)
    gt, gb, grad_input, dgain1 = grads(
        dims, n1, n2, dhb, g_all, dx, oc, wqkv, w_mine[1], w_mine[2], activations, dh, gains[:1]
    )

    grad_scale_local = dc[0, :HD] / factor * (SCALE_BASE / math.sqrt(HD)) * jax.nn.sigmoid(scale_param)
    parts = gb.reshape(6, data_par, own_rows, cols).transpose(1, 0, 2, 3)
    summed = scaling * lax.psum_scatter(parts, "dp", scatter_dimension=0).astype(F32)
    grad_in = summed[:4]
    grad_out = jnp.swapaxes(summed[4:], 1, 2)

    stored = scaling * gt + error_buffer[0]
    left_local = jnp.einsum("kcd,kcr->kdr", stored, factors, precision=HIGHEST)
    gain_local = scaling * jnp.concatenate([dgain1, dgain2])
    left, grad_gain, grad_scale = lax.psum(
        (left_local, gain_local, scaling * grad_scale_local), ("dp", "mp")
    )
    basis = orthonormal(left)
    right = lax.psum(jnp.einsum("kcd,kdr->kcr", stored, basis, precision=HIGHEST), "dp")
    error_new = (stored - jnp.einsum("kcr,kdr->kcd", right, basis, precision=HIGHEST))[None]
    mine_basis = lax.dynamic_slice_in_dim(basis, my_data * own_rows, own_rows, 1)
    mine = jnp.einsum("kdr,kcr->kdc", mine_basis, right, precision=HIGHEST)
    mom_in_new = MOMENTUM * mom_in + mine[:4]
    new_in = w_in - RATE * mom_in_new
    mom_out_new = MOMENTUM * mom_out + jnp.swapaxes(mine[4:], 1, 2)
    new_out = jnp.stack([w_attn_out, w_down]) - RATE * mom_out_new
    mom_gain_new = MOMENTUM * mom_gain + grad_gain
    new_gain = gains - RATE * mom_gain_new
    mom_scale_new = MOMENTUM * mom_scale + grad_scale
    new_scale = scale_param - RATE * mom_scale_new
    return (
        output, grad_input, grad_in, grad_out, grad_gain, grad_scale, new_in, new_out,
        new_gain, new_scale, mom_in_new, mom_out_new, mom_gain_new, mom_scale_new,
        error_new, right,
    )


def solution(mesh):
    tokens, shard = P(("dp", "mp"), None), P(None, "dp", "mp")
    return jax.shard_map(
        on_device,
        mesh=mesh,
        in_specs=(
            tokens, tokens, P("dp", None), shard, P("mp", "dp"), P("mp", "dp"), P(), P(),
            shard, P(None, "mp", "dp"), P(), P(), P("dp", None, "mp", None), P(None, "mp", None),
        ),
        out_specs=(
            tokens, tokens, shard, P(None, "mp", "dp"), P(), P(), shard, P(None, "mp", "dp"),
            P(), P(), shard, P(None, "mp", "dp"), P(), P(), P("dp", None, "mp", None),
            P(None, "mp", None),
        ),
        check_vma=False,
    )
```

```python
import functools
import math

import jax
import jax.numpy as jnp
from jax import lax
from jax.experimental import pallas as pl
from jax.experimental.pallas import tpu as pltpu
from jax.sharding import PartitionSpec as P

HD = 80
LANE = 128
HIGHEST = lax.Precision.HIGHEST
EPSILON = 1e-06
SCALE_BASE = 1.442695041
MOMENTUM = 0.9
RATE = 0.1
NEG = -1e30
F32 = jnp.float32
BF16 = jnp.bfloat16
MESH = pl.DeviceIdType.MESH
VMEM_LIMIT = 67_000_000


def nn(a, b):
    return jnp.dot(a, b, preferred_element_type=F32)


def nt(a, b):
    return lax.dot_general(a, b, (((1,), (1,)), ((), ())), preferred_element_type=F32)


def tn(a, b):
    return lax.dot_general(a, b, (((0,), (0,)), ((), ())), preferred_element_type=F32)


def spread(cols, heads):
    row = lax.broadcasted_iota(jnp.int32, (cols, heads * LANE), 0)
    col = lax.broadcasted_iota(jnp.int32, (cols, heads * LANE), 1)
    off = col & (LANE - 1)
    hit = (row == (col >> 7) * HD + off) & (off < HD)
    return jnp.where(hit, 1.0, 0.0).astype(BF16)


def block_rows(index, rows):
    return pl.ds(pl.multiple_of(index * rows, rows), rows)


def greet(peers):
    bar = pltpu.get_barrier_semaphore()
    for peer in peers:
        pl.semaphore_signal(bar, 1, device_id=peer, device_id_type=MESH)
    pl.semaphore_wait(bar, len(peers))


def line_peers(n, me):
    return [{"mp": lax.rem(me + off, n)} for off in range(1, n)]


class LineGather:
    def __init__(self, n, me, own, buf, ssem, rsem):
        self.n, self.me, self.own, self.buf = n, me, own, buf
        self.ssem, self.rsem = ssem, rsem

    def copy(self, slot, hop, way):
        src = self.own if hop == 0 else self.buf.at[slot]
        return pltpu.make_async_remote_copy(
            src_ref=src,
            dst_ref=self.buf.at[slot],
            send_sem=self.ssem.at[way, hop],
            recv_sem=self.rsem.at[slot],
            device_id={"mp": self.me + 1 - 2 * way},
            device_id_type=MESH,
        )

    def goes(self, hop, way):
        if way == 0:
            return (self.me - hop >= 0) & (self.me < self.n - 1)
        return (self.me + hop <= self.n - 1) & (self.me > 0)

    def slot(self, hop, way):
        return self.me - hop if way == 0 else self.me + hop

    def arrives(self, hop, way):
        return self.me - hop >= 0 if way == 0 else self.me + hop <= self.n - 1

    def send(self, hop, ways=(0, 1)):
        for way in ways:

            @pl.when(self.goes(hop, way))
            def _(way=way):
                self.copy(self.slot(hop, way), hop, way).start()

    def relay(self, hop):
        for way in (0, 1):

            @pl.when(self.arrives(hop, way))
            def _(way=way):
                slot = self.slot(hop, way)
                self.copy(slot, hop, way).wait_recv()

            if hop < self.n - 1:
                self.send(hop, (way,))

    def finish(self):
        for hop in range(self.n - 1):
            for way in (0, 1):

                @pl.when(self.goes(hop, way))
                def _(way=way, hop=hop):
                    self.copy(self.slot(hop, way), hop, way).wait_send()


def line_sems(n):
    return [pltpu.SemaphoreType.DMA((2, n)), pltpu.SemaphoreType.DMA((n,))]


def vmem(count):
    return [pl.BlockSpec(memory_space=pltpu.VMEM)] * count


def params(collective_id=None):
    return pltpu.CompilerParams(
        collective_id=collective_id,
        has_side_effects=collective_id is not None,
        vmem_limit_bytes=VMEM_LIMIT,
    )


def attend_kernel(
    dims, x_ref, w_ref, gain_ref, c_ref, st_ref,
    n1_ref, q_ref, k_ref, v_ref, lse_ref, oc_ref, of_ref,
    xbuf, wpad, mask, opad, zs, zr, as_, ar,
):
    n, rows, heads, span = dims
    me = lax.axis_index("mp")
    cols = w_ref.shape[2]
    greet(line_peers(n, me))
    gather = LineGather(n, me, x_ref, xbuf, zs, zr)
    gather.send(0)
    sel = spread(cols, heads)
    for m in range(3):
        wpad[m] = nn(w_ref[m], sel).astype(BF16)
    xbuf[me] = x_ref[...]

    def project(slot):
        x = xbuf[slot].astype(F32)
        scale = lax.rsqrt(jnp.mean(x * x, axis=-1, keepdims=True) + EPSILON)
        normed = (x * scale * gain_ref[...]).astype(BF16)
        n1_ref[slot] = normed
        at = block_rows(slot, rows)
        for m, ref in enumerate((q_ref, k_ref, v_ref)):
            out = nn(normed, wpad[m])
            if m == 0:
                out = out * c_ref[...]
            out = out.astype(BF16)
            for h in range(heads):
                ref[h, at, :] = out[:, h * LANE : (h + 1) * LANE]

    project(me)

    def arrivals(hop):
        def one(way, _):
            slot = me - hop + 2 * hop * way

            @pl.when((slot >= 0) & (slot < n))
            def _():
                project(slot)

            return 0

        lax.fori_loop(0, 2, one, 0)

    for hop in range(1, n):
        gather.relay(hop)
        arrivals(hop)

    def chunk(i, _):
        first = jnp.maximum(i - (span - 1), 0)
        at, keys = block_rows(i, rows), pl.ds(pl.multiple_of(first * rows, rows), span * rows)
        q_pos = i * rows + lax.broadcasted_iota(jnp.int32, mask.shape, 0)
        k_pos = first * rows + lax.broadcasted_iota(jnp.int32, mask.shape, 1)
        mask[...] = jnp.where((k_pos <= q_pos) & (k_pos >= st_ref[at, :]), 0.0, NEG)

        def head(h, _):
            scores = nt(q_ref[h, at, :], k_ref[h, keys, :]) + mask[...]
            top = jnp.max(scores, axis=-1, keepdims=True)
            raised = jnp.exp(scores - top)
            total = jnp.sum(raised, axis=-1, keepdims=True)
            prob = (raised * (1.0 / total)).astype(BF16)
            opad[h] = nn(prob, v_ref[h, keys, :]).astype(BF16)
            lse_ref[h, at, :] = top + jnp.log(total)
            return 0

        lax.fori_loop(0, heads, head, 0)
        wide = jnp.concatenate([opad[h] for h in range(heads)], axis=1)
        oc_ref[i] = nt(wide, sel).astype(BF16)

        @pl.when(i != me)
        def _():
            pltpu.make_async_remote_copy(
                src_ref=oc_ref.at[i], dst_ref=of_ref.at[me], send_sem=as_.at[i],
                recv_sem=ar.at[me], device_id={"mp": i}, device_id_type=MESH,
            ).start()

        @pl.when(i == me)
        def _():
            of_ref[me] = oc_ref[me]

        return 0

    lax.fori_loop(0, n, chunk, 0)
    gather.finish()
    for off in range(1, n):
        peer = lax.rem(me + off, n)
        copy = pltpu.make_async_remote_copy(
            src_ref=oc_ref.at[peer], dst_ref=of_ref.at[peer], send_sem=as_.at[peer],
            recv_sem=ar.at[peer], device_id={"mp": peer}, device_id_type=MESH,
        )
        copy.wait_send()
        copy.wait_recv()


def attend(dims, x, w, gain, c_row, starts):
    n, rows, heads, span = dims
    width, cols = x.shape[1], w.shape[2]
    count = n * rows
    head_out = jax.ShapeDtypeStruct((heads, count, LANE), BF16)
    return pl.pallas_call(
        functools.partial(attend_kernel, dims),
        out_shape=(
            jax.ShapeDtypeStruct((n, rows, width), BF16),
            head_out, head_out, head_out,
            jax.ShapeDtypeStruct((heads, count, 1), F32),
            jax.ShapeDtypeStruct((n, rows, cols), BF16),
            jax.ShapeDtypeStruct((n, rows, cols), BF16),
        ),
        in_specs=vmem(5),
        out_specs=vmem(7),
        scratch_shapes=[
            pltpu.VMEM((n, rows, width), BF16),
            pltpu.VMEM((3, width, heads * LANE), BF16),
            pltpu.VMEM((rows, span * rows), F32),
            pltpu.VMEM((heads, rows, LANE), BF16),
            *line_sems(n),
            pltpu.SemaphoreType.DMA((n,)),
            pltpu.SemaphoreType.DMA((n,)),
        ],
        compiler_params=params(1),
        name="attend",
    )(x, w, gain, c_row, starts)


def middle_kernel(
    dims, x_ref, g_ref, of_ref, w_ref, gain_ref,
    out_ref, dh_ref, n2_ref, g_all, dhb_ref, dgain_ref,
    h_ref, acc, dn2, gs, gr, ns, nr, ds, dr,
):
    n = dims[0]
    me = lax.axis_index("mp")
    greet(line_peers(n, me))
    gather_g = LineGather(n, me, g_ref, g_all, gs, gr)
    gather_n = LineGather(n, me, n2_ref.at[me], n2_ref, ns, nr)
    gather_d = LineGather(n, me, dhb_ref.at[me], dhb_ref, ds, dr)
    gather_g.send(0)
    g_all[me] = g_ref[...]
    h_ref[...] = x_ref[...].astype(F32)

    def project(j, _):
        h_ref[...] += nt(of_ref[j], w_ref[j, 0])
        return 0

    lax.fori_loop(0, n, project, 0)
    h = h_ref[...]
    scale = lax.rsqrt(jnp.mean(h * h, axis=-1, keepdims=True) + EPSILON)
    n2_ref[me] = (h * scale * gain_ref[...]).astype(BF16)
    gather_n.send(0)
    acc[...] = h_ref[...]
    dn2[...] = jnp.zeros_like(dn2)

    def hidden(j, _):
        gate = nn(n2_ref[me], w_ref[j, 1])
        sig = 1.0 / (1.0 + jnp.exp(-gate))
        acc[...] += nt((gate * sig).astype(BF16), w_ref[j, 2])
        dz = nn(g_ref[...], w_ref[j, 2])
        da = (dz * (sig * (1.0 + gate * (1.0 - sig)))).astype(BF16)
        dn2[...] += nt(da, w_ref[j, 1])
        return 0

    lax.fori_loop(0, n, hidden, 0)
    out_ref[...] = acc[...].astype(BF16)
    h = h_ref[...]
    scale = lax.rsqrt(jnp.mean(h * h, axis=-1, keepdims=True) + EPSILON)
    unit = h * scale
    grad = dn2[...]
    dgain_ref[...] = jnp.sum(grad * unit, axis=0, keepdims=True)
    du = grad * gain_ref[...]
    dh = g_ref[...].astype(F32) + scale * (du - unit * jnp.mean(du * unit, axis=-1, keepdims=True))
    dh_ref[...] = dh
    dhb_ref[me] = dh.astype(BF16)
    gather_d.send(0)
    for hop in range(1, n):
        gather_g.relay(hop)
        gather_n.relay(hop)
        gather_d.relay(hop)
    for gather in (gather_g, gather_n, gather_d):
        gather.finish()


def middle(dims, x, g, o_full, w_full, gain):
    n, rows = dims[:2]
    width = x.shape[1]
    every = jax.ShapeDtypeStruct((n, rows, width), BF16)
    return pl.pallas_call(
        functools.partial(middle_kernel, dims),
        out_shape=(
            jax.ShapeDtypeStruct((rows, width), BF16),
            jax.ShapeDtypeStruct((rows, width), F32),
            every, every, every,
            jax.ShapeDtypeStruct((1, width), F32),
        ),
        in_specs=vmem(5),
        out_specs=vmem(6),
        scratch_shapes=[pltpu.VMEM((rows, width), F32)] * 3 + line_sems(n) * 3,
        compiler_params=params(2),
        name="middle",
    )(x, g, o_full, w_full, gain)


def back_kernel(
    dims, q_ref, k_ref, v_ref, lse_ref, dhb_ref, w_ref, c_ref, st_ref,
    dx_ref, dc_ref,
    wpad, mask, do_ref, dq_ref, dk_ref, dv_ref,
):
    n, rows, heads, span = dims
    sel = spread(w_ref.shape[1], heads)
    wpad[...] = nn(w_ref[...], sel).astype(BF16)
    dk_ref[...] = jnp.zeros_like(dk_ref)
    dv_ref[...] = jnp.zeros_like(dv_ref)
    dc_ref[...] = jnp.zeros_like(dc_ref)

    def squeeze(ref, at):
        wide = jnp.concatenate([ref[h, at, :].astype(BF16) for h in range(heads)], axis=1)
        return nt(wide, sel).astype(BF16)

    def chunk(i, _):
        first = jnp.maximum(i - (span - 1), 0)
        at, keys = block_rows(i, rows), pl.ds(pl.multiple_of(first * rows, rows), span * rows)
        q_pos = i * rows + lax.broadcasted_iota(jnp.int32, mask.shape, 0)
        k_pos = first * rows + lax.broadcasted_iota(jnp.int32, mask.shape, 1)
        mask[...] = jnp.where((k_pos <= q_pos) & (k_pos >= st_ref[at, :]), 0.0, NEG)
        grad = nn(dhb_ref[i], wpad[...]).astype(BF16)
        for h in range(heads):
            do_ref[h] = grad[:, h * LANE : (h + 1) * LANE]

        def head(h, _):
            query = q_ref[h, at, :]
            scores = nt(query, k_ref[h, keys, :]) + mask[...]
            prob = jnp.exp(scores - lse_ref[h, at, :])
            dp = nt(do_ref[h], v_ref[h, keys, :])
            inner = jnp.sum(prob * dp, axis=-1, keepdims=True)
            ds = (prob * (dp - inner)).astype(BF16)
            dq = nn(ds, k_ref[h, keys, :])
            dk_ref[h, keys, :] += tn(ds, query)
            dv_ref[h, keys, :] += tn(prob.astype(BF16), do_ref[h])
            dc_ref[...] += jnp.sum(dq * query.astype(F32), axis=0, keepdims=True)
            dq_ref[h] = (dq * c_ref[:, :LANE]).astype(BF16)
            return 0

        lax.fori_loop(0, heads, head, 0)
        dx_ref[0, i] = squeeze(dq_ref, slice(None))
        return 0

    lax.fori_loop(0, n, chunk, 0)

    def close(i, _):
        at = block_rows(i, rows)
        dx_ref[1, i] = squeeze(dk_ref, at)
        dx_ref[2, i] = squeeze(dv_ref, at)
        return 0

    lax.fori_loop(0, n, close, 0)


def back(dims, q, k, v, lse, dhb, w_out, c_row, starts):
    n, rows, heads, span = dims
    cols, width = w_out.shape[1], w_out.shape[0]
    return pl.pallas_call(
        functools.partial(back_kernel, dims),
        out_shape=(
            jax.ShapeDtypeStruct((3, n, rows, cols), BF16),
            jax.ShapeDtypeStruct((1, LANE), F32),
        ),
        in_specs=vmem(8),
        out_specs=vmem(2),
        scratch_shapes=[
            pltpu.VMEM((width, heads * LANE), BF16),
            pltpu.VMEM((rows, span * rows), F32),
            pltpu.VMEM((heads, rows, LANE), BF16),
            pltpu.VMEM((heads, rows, LANE), BF16),
            pltpu.VMEM((heads, n * rows, LANE), F32),
            pltpu.VMEM((heads, n * rows, LANE), F32),
        ],
        compiler_params=params(),
        name="back",
    )(q, k, v, lse, dhb, w_out, c_row, starts)


def halves(value):
    high = value.astype(BF16)
    return high, (value - high.astype(F32)).astype(BF16)


def dot_split(small, big, contract):
    count = small.shape[0]
    high, low = halves(small)
    big_high, big_low = halves(big)
    both = contract(jnp.concatenate([high.astype(F32), low.astype(F32)], axis=0).astype(BF16), big_high)
    return both[:count] + both[count:] + contract(high, big_low)


def plane(data_par):
    half = data_par // 2
    side = math.isqrt(half)
    return (side, half // side) if side * side == half else (1, half)


class PlaneScatter:
    def __init__(self, n_data, gb, core, a1, b1, a2, b2, sems):
        self.ys, self.xs = plane(n_data)
        self.gb, self.core, self.a1, self.b1, self.a2, self.b2 = gb, core, a1, b1, a2, b2
        (self.c_s, self.c_r, self.s1, self.ra1, self.rb1, self.s2, self.ra2, self.rb2) = sems
        me = lax.axis_index("dp")
        self.c = lax.rem(me, 2)
        self.x = lax.rem(me // 2, self.xs)
        self.y = me // (2 * self.xs)
        self.half = gb.shape[0] // 2

    def send(self, src, dst, ssem, rsem, y, x, c):
        return pltpu.make_async_remote_copy(
            src_ref=src, dst_ref=dst, send_sem=ssem, recv_sem=rsem,
            device_id={"dp": (y * self.xs + x) * 2 + c}, device_id_type=MESH,
        )

    def copies_core(self):
        other = 1 - self.c
        src = self.gb.at[:, :, :, other]
        return [self.send(src, self.core, self.c_s, self.c_r, self.y, self.x, other)]

    def copies_one(self):
        out, h = [], self.half
        for o in range(1, self.xs):
            to = lax.rem(self.x + o, self.xs)
            src = self.core.at[:h, :, to]
            out.append(self.send(src, self.a1.at[o - 1], self.s1.at[0, o], self.ra1.at[o], self.y, to, self.c))
        for o in range(1, self.ys):
            to = lax.rem(self.y + o, self.ys)
            src = self.core.at[h:, to]
            out.append(self.send(src, self.b1.at[o - 1], self.s1.at[1, o], self.rb1.at[o], to, self.x, self.c))
        return out

    def copies_two(self):
        out, h = [], self.half
        for o in range(1, self.ys):
            to = lax.rem(self.y + o, self.ys)
            src = self.core.at[:h, to, self.x]
            out.append(self.send(src, self.a2.at[o - 1], self.s2.at[0, o], self.ra2.at[o], to, self.x, self.c))
        for o in range(1, self.xs):
            to = lax.rem(self.x + o, self.xs)
            src = self.core.at[h:, self.y, to]
            out.append(self.send(src, self.b2.at[o - 1], self.s2.at[1, o], self.rb2.at[o], self.y, to, self.c))
        return out

    def start(self, copies):
        for copy in copies:
            copy.start()

    def arrive(self, copies):
        for copy in copies:
            copy.wait_recv()

    def sum_core(self):
        self.arrive(self.copies_core())

        def one(i, _):
            m, rest = i // (self.ys * self.xs), lax.rem(i, self.ys * self.xs)
            y, x = rest // self.xs, lax.rem(rest, self.xs)
            total = self.core[m, y, x].astype(F32) + self.gb[m, y, x, self.c].astype(F32)
            self.core[m, y, x] = total.astype(BF16)
            return 0

        lax.fori_loop(0, self.gb.shape[0] * self.ys * self.xs, one, 0)

    def sum_one(self):
        self.arrive(self.copies_one())
        h = self.half

        def along_y(i, _):
            m, y = i // self.ys, lax.rem(i, self.ys)
            total = self.core[m, y, self.x].astype(F32)
            for o in range(1, self.xs):
                total += self.a1[o - 1, m, y].astype(F32)
            self.core[m, y, self.x] = total.astype(BF16)
            return 0

        def along_x(i, _):
            m, x = i // self.xs, lax.rem(i, self.xs)
            total = self.core[h + m, self.y, x].astype(F32)
            for o in range(1, self.ys):
                total += self.b1[o - 1, m, x].astype(F32)
            self.core[h + m, self.y, x] = total.astype(BF16)
            return 0

        lax.fori_loop(0, h * self.ys, along_y, 0)
        lax.fori_loop(0, h * self.xs, along_x, 0)

    def sum_two(self, out, factor):
        self.arrive(self.copies_two())
        h = self.half

        def one(m, _):
            total = self.core[m, self.y, self.x].astype(F32)
            for o in range(1, self.ys):
                total += self.a2[o - 1, m].astype(F32)
            out[m] = factor * total
            total = self.core[h + m, self.y, self.x].astype(F32)
            for o in range(1, self.xs):
                total += self.b2[o - 1, m].astype(F32)
            out[h + m] = factor * total
            return 0

        lax.fori_loop(0, h, one, 0)

    def finish(self):
        for copy in self.copies_core() + self.copies_one() + self.copies_two():
            copy.wait_send()

    @staticmethod
    def scratch(n_data, count, rows, cols):
        ys, xs = plane(n_data)
        h = count // 2
        sem = pltpu.SemaphoreType.DMA
        return [
            pltpu.VMEM((count, ys, xs, 2, rows, cols), BF16),
            pltpu.VMEM((count, ys, xs, rows, cols), BF16),
            pltpu.VMEM((max(xs - 1, 1), h, ys, rows, cols), BF16),
            pltpu.VMEM((max(ys - 1, 1), h, xs, rows, cols), BF16),
            pltpu.VMEM((max(ys - 1, 1), h, rows, cols), BF16),
            pltpu.VMEM((max(xs - 1, 1), h, rows, cols), BF16),
            sem, sem, sem((2, max(xs, ys))), sem((xs,)), sem((ys,)),
            sem((2, max(xs, ys))), sem((ys,)), sem((xs,)),
        ]


class Exchange:
    def __init__(self, axis, size, src_of, dst, ssem, rsem):
        self.axis, self.size, self.src_of, self.dst, self.ssem, self.rsem = axis, size, src_of, dst, ssem, rsem
        self.me = lax.axis_index(axis)

    def copy(self, peer, slot):
        return pltpu.make_async_remote_copy(
            src_ref=self.src_of(peer), dst_ref=self.dst.at[slot], send_sem=self.ssem.at[peer],
            recv_sem=self.rsem.at[slot], device_id={self.axis: peer}, device_id_type=MESH,
        )

    def each(self, do):
        def one(off, _):
            do(lax.rem(self.me + off, self.size))
            return 0

        lax.fori_loop(1, self.size, one, 0)

    def start(self):
        self.each(lambda peer: self.copy(peer, self.me).start())

    def arrive(self):
        self.each(lambda peer: self.copy(peer, peer).wait_recv())

    def finish(self):
        self.each(lambda peer: self.copy(peer, peer).wait_send())


def total_of(ref, size):
    def one(i, total):
        return total + ref[i]

    return lax.fori_loop(1, size, one, ref[0])


def grads_kernel(
    dims, n_data, scaling, n1_ref, n2_ref, dhb_ref, g_ref, dx_ref, oc_ref, wqkv_ref, wup_ref, wdn_ref,
    x_ref, dh_ref, gain_ref, dgain2_ref, dscale_ref, ft_ref, err_ref,
    gsum_ref, gin_ref, m_out, basis_ref, right_ref, small_ref,
    abuf, z_ref, da_ref, sbuf, lbuf, m_ref, lsend, lrecv, zrecv, lfull, rrecv, srecv, szrecv,
    fs, ss, ls, es, ms, l_s, l_r, z_s, z_r, a_s, a_r, r_s, r_r, g_s, g_r, gz_s, gz_r, *plane_refs,
):
    n, rows, heads, span = dims
    me, mine = lax.axis_index("mp"), lax.axis_index("dp")
    width, cols = wup_ref.shape
    tiles = width // LANE

    def load(m):
        return pltpu.make_async_copy(err_ref.at[m], m_ref.at[m], es.at[m])

    def save(m):
        return pltpu.make_async_copy(m_ref.at[m], m_out.at[m], ms.at[m])

    def fetch(k):
        src = (n2_ref, g_ref, dhb_ref, n1_ref)[k]
        return pltpu.make_async_copy(src, abuf.at[k % 2], fs.at[k])

    fetch(0).start()
    fetch(1).start()
    for m in range(6):
        load(m).start()
    greet(line_peers(n, me) + [{"dp": lax.rem(mine + off, n_data)} for off in range(1, n_data)])
    scatter = PlaneScatter(n_data, *plane_refs[:6], plane_refs[6:])
    gb = plane_refs[0]
    ex_left = Exchange("dp", n_data, lambda peer: lsend.at[peer], lrecv, l_s, l_r)
    ex_line = Exchange("mp", n, lambda peer: zrecv.at[me], zrecv, z_s, z_r)
    ex_all = Exchange("dp", n_data, lambda peer: lfull.at[mine], lfull, a_s, a_r)
    ex_right = Exchange("dp", n_data, lambda peer: rrecv.at[mine], rrecv, r_s, r_r)
    ex_small = Exchange("dp", n_data, lambda peer: srecv.at[mine], srecv, g_s, g_r)
    ex_small_line = Exchange("mp", n, lambda peer: szrecv.at[me], szrecv, gz_s, gz_r)


    def own(e, _):
        i = jnp.where(lax.rem(e, 2) == 0, n - 1 - e // 2, e // 2)
        total = nt(dx_ref[0, i], wqkv_ref[0])
        total += nt(dx_ref[1, i], wqkv_ref[1])
        total += nt(dx_ref[2, i], wqkv_ref[2])

        @pl.when(i == me)
        def _():
            gin_ref[...] = total

        @pl.when(i != me)
        def _():
            sbuf[i] = total.astype(BF16)

        return 0

    lax.fori_loop(0, n, own, 0)

    def copy(i, way, here=False):
        slot = i if way == 0 else jnp.where(i == (me if here else me - 1), n, i)
        return pltpu.make_async_remote_copy(
            src_ref=sbuf.at[i], dst_ref=lbuf.at[slot], send_sem=ss.at[i], recv_sem=ls.at[slot],
            device_id={"mp": me + 1 - 2 * way}, device_id_type=MESH,
        )

    def launch():
        @pl.when(me == 0)
        def _():
            for i in range(n - 1, 0, -1):
                copy(i, 0).start()

        @pl.when(me == n - 1)
        def _():
            for i in range(n - 1):
                copy(i, 1).start()

    def relay(r):
        for way in (0, 1):
            place = me if way == 0 else n - 1 - me
            i = n - 1 - r + me if way == 0 else r - (n - 1 - me)

            @pl.when((place >= 1) & (place <= r))
            def _(i=i, way=way):
                copy(i, way, True).wait_recv()
                sbuf[i] = (sbuf[i].astype(F32) + lbuf[i].astype(F32)).astype(BF16)
                copy(i, way).start()

    launch()

    def hidden(i, _):
        gate = nn(abuf[0, i], wup_ref[...])
        sig = 1.0 / (1.0 + jnp.exp(-gate))
        z_ref[i] = (gate * sig).astype(BF16)
        dz = nn(abuf[1, i], wdn_ref[...])
        da_ref[i] = (dz * (sig * (1.0 + gate * (1.0 - sig)))).astype(BF16)
        return 0

    def flat(value):
        return value.reshape(n * rows, value.shape[-1])

    def weight(m, a, b):
        left, right = flat(a), flat(b)
        load(m).wait()
        m_ref[m] = scaling * tn(right, left) + m_ref[m]
        gb[m] = tn(left, right).reshape(gb.shape[1:]).astype(BF16)

    def factor_rows(m):
        rows_left = dot_split(ft_ref[m], m_ref[m], nn)
        per = lsend.shape[1]
        for t in range(tiles):
            tile = m * tiles + t
            lsend[tile // per, lax.rem(tile, per)] = rows_left[:, t * LANE : (t + 1) * LANE]

    fetch(0).wait()
    fetch(1).wait()
    lax.fori_loop(0, n, hidden, 0)
    weight(3, abuf[0], da_ref[...])
    fetch(2).start()
    weight(5, abuf[1], z_ref[...])
    fetch(3).start()
    fetch(2).wait()
    weight(4, abuf[0], oc_ref[...])
    relay(1)
    fetch(3).wait()

    def inputs(m, _):
        weight(m, abuf[1], dx_ref[m])
        return 0

    lax.fori_loop(0, 3, inputs, 0)
    for tile in range(6 * tiles, lsend.shape[0] * lsend.shape[1]):
        lsend[tile // lsend.shape[1], tile % lsend.shape[1]] = jnp.zeros((8, LANE), F32)

    def left_rows(m, _):
        factor_rows(m)
        return 0

    lax.fori_loop(0, 6, left_rows, 0)
    lrecv[mine] = lsend[mine]
    ex_left.start()
    scatter.start(scatter.copies_core())
    for m in range(6):
        save(m).start()
    ex_left.arrive()
    zrecv[me] = total_of(lrecv, n_data)
    ex_line.start()
    for r in range(2, n - 1):
        relay(r)
    scatter.sum_core()
    scatter.start(scatter.copies_one())
    ex_line.arrive()
    lfull[mine] = total_of(zrecv, n)
    ex_all.start()
    ex_all.arrive()

    per = lfull.shape[1]
    basis = jnp.stack(
        [
            jnp.concatenate([lfull[t // per, t % per] for t in range(m * tiles, (m + 1) * tiles)], axis=1)
            for m in range(6)
        ]
    )
    row = lax.broadcasted_iota(jnp.int32, (1, 8, 1), 1)
    for index in range(8):
        vector = basis[:, index : index + 1, :]
        vector = vector * lax.rsqrt(jnp.sum(vector * vector, axis=-1, keepdims=True) + 1e-12)
        onto = jnp.where(row > index, jnp.sum(basis * vector, axis=-1, keepdims=True), 0.0)
        basis = jnp.where(row == index, vector, basis - onto * vector)
    basis_ref[...] = basis

    def right_rows(m, _):
        rrecv[mine, m] = dot_split(basis_ref[m], m_ref[m], nt)
        return 0

    lax.fori_loop(0, 6, right_rows, 0)
    ex_right.start()
    scatter.sum_one()
    scatter.start(scatter.copies_two())


    @pl.when(me > 0)
    def _():
        copy(me, 0).wait_recv()
        gin_ref[...] += lbuf[me].astype(F32)

    @pl.when(me < n - 1)
    def _():
        copy(me, 1, True).wait_recv()
        gin_ref[...] += lbuf[n].astype(F32)

    x = x_ref[...].astype(F32)
    scale = lax.rsqrt(jnp.mean(x * x, axis=-1, keepdims=True) + EPSILON)
    unit = x * scale
    grad = gin_ref[...]
    dgain = jnp.sum(grad * unit, axis=0, keepdims=True)
    srecv[mine] = jnp.zeros(srecv.shape[1:], F32)
    for t in range(tiles):
        at = slice(t * LANE, (t + 1) * LANE)
        srecv[mine, t // 8, t % 8 : t % 8 + 1, :] = scaling * dgain[:, at]
        t2 = tiles + t
        srecv[mine, t2 // 8, t2 % 8 : t2 % 8 + 1, :] = scaling * dgain2_ref[:, at]
    t3 = 2 * tiles
    srecv[mine, t3 // 8, t3 % 8 : t3 % 8 + 1, :] = scaling * dscale_ref[...]
    ex_small.start()
    du = grad * gain_ref[...]
    gin_ref[...] = dh_ref[...] + scale * (du - unit * jnp.mean(du * unit, axis=-1, keepdims=True))
    ex_small.arrive()
    szrecv[me] = total_of(srecv, n_data)
    ex_small_line.start()
    ex_right.arrive()
    right_ref[...] = total_of(rrecv, n_data)
    scatter.sum_two(gsum_ref, scaling)
    ex_small_line.arrive()
    small_ref[...] = total_of(szrecv, n)

    for i in range(n):

        @pl.when(me < i)
        def _(i=i):
            copy(i, 0).wait_send()

        @pl.when(me > i)
        def _(i=i):
            copy(i, 1).wait_send()

    for exchange in (ex_left, ex_line, ex_all, ex_right, ex_small, ex_small_line):
        exchange.finish()
    scatter.finish()
    for m in range(6):
        save(m).wait()


def grads(dims, scaling, n1, n2, dhb, g_all, dx, oc, wqkv, w_up, w_down, x, dh, gain, dgain2, dscale, ft, err):
    n, rows = dims[:2]
    n_data = lax.axis_size("dp")
    width, cols = w_up.shape
    own_rows = width // n_data
    every = pltpu.VMEM((n, rows, width), BF16)
    sem = pltpu.SemaphoreType.DMA
    per = -(-(6 * width // LANE) // n_data)
    small = -(-(2 * width // LANE + 1) // 8)

    def f32(*shape):
        return pltpu.VMEM(shape, F32)

    return pl.pallas_call(
        functools.partial(grads_kernel, dims, n_data, scaling),
        out_shape=(
            jax.ShapeDtypeStruct((6, own_rows, cols), F32),
            jax.ShapeDtypeStruct((rows, width), F32),
            jax.ShapeDtypeStruct((6, cols, width), F32),
            jax.ShapeDtypeStruct((6, 8, width), F32),
            jax.ShapeDtypeStruct((6, 8, cols), F32),
            jax.ShapeDtypeStruct((small, 8, LANE), F32),
        ),
        in_specs=[pl.BlockSpec(memory_space=pl.ANY)] * 4 + vmem(11) + [pl.BlockSpec(memory_space=pl.ANY)],
        out_specs=vmem(2) + [pl.BlockSpec(memory_space=pl.ANY)] + vmem(3),
        scratch_shapes=[
            pltpu.VMEM((2, n, rows, width), BF16),
            pltpu.VMEM((n, rows, cols), BF16),
            pltpu.VMEM((n, rows, cols), BF16),
            every,
            pltpu.VMEM((n + 1, rows, width), BF16),
            f32(6, cols, width),
            f32(n_data, per, 8, LANE), f32(n_data, per, 8, LANE), f32(n, per, 8, LANE),
            f32(n_data, per, 8, LANE), f32(n_data, 6, 8, cols),
            f32(n_data, small, 8, LANE), f32(n, small, 8, LANE),
            sem((4,)), sem((n,)), sem((n + 1,)), sem((6,)), sem((6,)),
            sem((n_data,)), sem((n_data,)), sem((n,)), sem((n,)), sem((n_data,)), sem((n_data,)),
            sem((n_data,)), sem((n_data,)), sem((n_data,)), sem((n_data,)), sem((n,)), sem((n,)),
            *PlaneScatter.scratch(n_data, 6, own_rows, cols),
        ],
        compiler_params=params(3),
        name="grads",
    )(n1, n2, dhb, g_all, dx, oc, wqkv, w_up, w_down, x, dh, gain, dgain2, dscale, ft, err)


def close_kernel(m_ref, right_ref, basis_ref, out_ref):
    right, basis = right_ref[0], basis_ref[0]
    (rh, rl), (bh, bl) = halves(right), halves(basis)
    left = jnp.concatenate([rh, rl, rh], axis=0)
    out_ref[0] = m_ref[0] - tn(left, jnp.concatenate([bh, bh, bl], axis=0))


def close(m, right, basis):
    cols, width = m.shape[1:]

    def spec(*shape):
        return pl.BlockSpec((1, *shape), lambda i: (i, 0, 0))

    return pl.pallas_call(
        close_kernel,
        grid=(6,),
        out_shape=jax.ShapeDtypeStruct(m.shape, F32),
        in_specs=[spec(cols, width), spec(8, cols), spec(8, width)],
        out_specs=spec(cols, width),
        compiler_params=params(),
        name="close",
    )(m, right, basis)


def on_device(
    activations, cotangent, doc_lengths, w_in, w_attn_out, w_down, gains, scale_param,
    mom_in, mom_out, mom_gain, mom_scale, error_buffer, factors,
):
    rows, width = activations.shape
    n = lax.axis_size("mp")
    data_par = lax.axis_size("dp")
    my_data, me = lax.axis_index("dp"), lax.axis_index("mp")
    count = rows * n
    scaling = (count * data_par) ** (-0.5)
    cols = w_in.shape[2]
    own_rows = w_in.shape[1]
    heads = cols // HD
    longest = count // 2
    span = min(n, -(-(longest - 1) // rows) + 1)
    dims = (n, rows, heads, span)

    shards = jnp.concatenate([w_in, w_attn_out.T[None], w_down.T[None]], axis=0).astype(BF16)
    wqkv = lax.all_gather(shards[:3], "dp", axis=1, tiled=True)
    tail = jnp.stack([shards[4], shards[3], shards[5]])
    w_full = lax.all_gather(lax.all_gather(tail, "mp", axis=0), "dp", axis=2, tiled=True)
    w_mine = lax.dynamic_index_in_dim(w_full, me, 0, keepdims=False)

    ends = jnp.cumsum(doc_lengths[0])
    position = jnp.arange(count, dtype=jnp.int32)[:, None]
    starts = jnp.max(jnp.where(ends[None, :] <= position, ends[None, :], 0), axis=1, keepdims=True)
    factor = SCALE_BASE / math.sqrt(HD) * jax.nn.softplus(scale_param)
    c_row = jnp.tile(jnp.pad(factor, (0, LANE - HD)), heads)[None]

    n1, q, k, v, lse, oc, o_full = attend(dims, activations, wqkv, gains[:1], c_row, starts)
    output, dh, n2, g_all, dhb, dgain2 = middle(dims, activations, cotangent, o_full, w_full, gains[1:])
    dx, dc = back(dims, q, k, v, lse, dhb, w_mine[0], c_row, starts)
    grad_scale_local = dc[0, :HD] / factor * (SCALE_BASE / math.sqrt(HD)) * jax.nn.sigmoid(scale_param)
    dscale = jnp.pad(grad_scale_local, (0, LANE - HD))[None]
    summed, grad_input, stored, basis, right, small = grads(
        dims, scaling, n1, n2, dhb, g_all, dx, oc, wqkv, w_mine[1], w_mine[2], activations, dh, gains[:1],
        dgain2, dscale, jnp.swapaxes(factors, 1, 2), error_buffer[0],
    )
    grad_in = summed[:4]
    grad_out = jnp.swapaxes(summed[4:], 1, 2)
    error_new = close(stored, right, basis)[None]
    tiles = width // LANE
    small = small.reshape(-1, LANE)
    grad_gain = small[: 2 * tiles].reshape(2, width)
    grad_scale = small[2 * tiles, :HD]
    mine_basis = lax.dynamic_slice_in_dim(basis, my_data * own_rows, own_rows, 2)
    mine = jnp.einsum("krd,krc->kdc", mine_basis, right, precision=HIGHEST)
    right = jnp.swapaxes(right, 1, 2)
    mom_in_new = MOMENTUM * mom_in + mine[:4]
    new_in = w_in - RATE * mom_in_new
    mom_out_new = MOMENTUM * mom_out + jnp.swapaxes(mine[4:], 1, 2)
    new_out = jnp.stack([w_attn_out, w_down]) - RATE * mom_out_new
    mom_gain_new = MOMENTUM * mom_gain + grad_gain
    new_gain = gains - RATE * mom_gain_new
    mom_scale_new = MOMENTUM * mom_scale + grad_scale
    new_scale = scale_param - RATE * mom_scale_new
    return (
        output, grad_input, grad_in, grad_out, grad_gain, grad_scale, new_in, new_out,
        new_gain, new_scale, mom_in_new, mom_out_new, mom_gain_new, mom_scale_new,
        error_new, right,
    )


def solution(mesh):
    tokens, shard = P(("dp", "mp"), None), P(None, "dp", "mp")
    return jax.shard_map(
        on_device,
        mesh=mesh,
        in_specs=(
            tokens, tokens, P("dp", None), shard, P("mp", "dp"), P("mp", "dp"), P(), P(),
            shard, P(None, "mp", "dp"), P(), P(), P("dp", None, "mp", None), P(None, "mp", None),
        ),
        out_specs=(
            tokens, tokens, shard, P(None, "mp", "dp"), P(), P(), shard, P(None, "mp", "dp"),
            P(), P(), shard, P(None, "mp", "dp"), P(), P(), P("dp", None, "mp", None),
            P(None, "mp", None),
        ),
        check_vma=False,
    )
```

```python
import functools
import math

import jax
import jax.numpy as jnp
from jax import lax
from jax.experimental import pallas as pl
from jax.experimental.pallas import tpu as pltpu
from jax.sharding import PartitionSpec as P

HD = 80
LANE = 128
HIGHEST = lax.Precision.HIGHEST
EPSILON = 1e-06
SCALE_BASE = 1.442695041
MOMENTUM = 0.9
RATE = 0.1
NEG = -1e30
F32 = jnp.float32
BF16 = jnp.bfloat16
MESH = pl.DeviceIdType.MESH
VMEM_LIMIT = 67_000_000


def nn(a, b):
    return jnp.dot(a, b, preferred_element_type=F32)


def nt(a, b):
    return lax.dot_general(a, b, (((1,), (1,)), ((), ())), preferred_element_type=F32)


def tn(a, b):
    return lax.dot_general(a, b, (((0,), (0,)), ((), ())), preferred_element_type=F32)


def spread(cols, heads):
    row = lax.broadcasted_iota(jnp.int32, (cols, heads * LANE), 0)
    col = lax.broadcasted_iota(jnp.int32, (cols, heads * LANE), 1)
    off = col & (LANE - 1)
    hit = (row == (col >> 7) * HD + off) & (off < HD)
    return jnp.where(hit, 1.0, 0.0).astype(BF16)


def block_rows(index, rows):
    return pl.ds(pl.multiple_of(index * rows, rows), rows)


def greet(peers):
    bar = pltpu.get_barrier_semaphore()
    for peer in peers:
        pl.semaphore_signal(bar, 1, device_id=peer, device_id_type=MESH)
    pl.semaphore_wait(bar, len(peers))


def line_peers(n, me):
    return [{"mp": lax.rem(me + off, n)} for off in range(1, n)]


class LineGather:
    def __init__(self, n, me, source, buf, ssem, rsem):
        self.n, self.me, self.source, self.buf = n, me, source, buf
        self.ssem, self.rsem = ssem, rsem

    def copy(self, slot, hop, way):
        return pltpu.make_async_remote_copy(
            src_ref=self.source(hop, slot),
            dst_ref=self.buf.at[slot],
            send_sem=self.ssem.at[way, hop],
            recv_sem=self.rsem.at[slot],
            device_id={"mp": self.me + 1 - 2 * way},
            device_id_type=MESH,
        )

    def goes(self, hop, way):
        if way == 0:
            return (self.me - hop >= 0) & (self.me < self.n - 1)
        return (self.me + hop <= self.n - 1) & (self.me > 0)

    def slot(self, hop, way):
        return self.me - hop if way == 0 else self.me + hop

    def arrives(self, hop, way):
        return self.me - hop >= 0 if way == 0 else self.me + hop <= self.n - 1

    def send(self, hop, ways=(0, 1)):
        for way in ways:

            @pl.when(self.goes(hop, way))
            def _(way=way):
                self.copy(self.slot(hop, way), hop, way).start()

    def take(self, hop, ways=(0, 1)):
        for way in ways:

            @pl.when(self.arrives(hop, way))
            def _(way=way):
                self.copy(self.slot(hop, way), hop, way).wait_recv()

    def relay(self, hop):
        for way in (0, 1):
            self.take(hop, (way,))
            if hop < self.n - 1:
                self.send(hop, (way,))

    def finish(self, first=0, last=None):
        for hop in range(first, self.n - 1 if last is None else last):
            for way in (0, 1):

                @pl.when(self.goes(hop, way))
                def _(way=way, hop=hop):
                    self.copy(self.slot(hop, way), hop, way).wait_send()


def own_then(own, buf):
    return lambda hop, slot: own if hop == 0 else buf.at[slot]


def line_sems(n):
    return [pltpu.SemaphoreType.DMA((2, n)), pltpu.SemaphoreType.DMA((n,))]


def vmem(count):
    return [pl.BlockSpec(memory_space=pltpu.VMEM)] * count


def params(collective_id=None):
    return pltpu.CompilerParams(
        collective_id=collective_id,
        has_side_effects=collective_id is not None,
        vmem_limit_bytes=VMEM_LIMIT,
    )


def plane(data_par):
    half = data_par // 2
    side = math.isqrt(half)
    return (side, half // side) if side * side == half else (1, half)


class PlaneGather:
    def __init__(self, n_data, buf, sems):
        self.ys, self.xs = plane(n_data)
        self.buf = buf
        self.s1a, self.s1b, self.r1a, self.r1b, self.s2a, self.s2b, self.r2a, self.r2b, self.cs, self.cr = sems
        me = lax.axis_index("dp")
        self.c = lax.rem(me, 2)
        self.x = lax.rem(me // 2, self.xs)
        self.y = me // (2 * self.xs)

    def move(self, src, dst, ssem, rsem, y, x, c):
        return pltpu.make_async_remote_copy(
            src_ref=src, dst_ref=dst, send_sem=ssem, recv_sem=rsem,
            device_id={"dp": (y * self.xs + x) * 2 + c}, device_id_type=MESH,
        )

    def east(self, o):
        return lax.rem(self.x + o + self.xs, self.xs)

    def north(self, o):
        return lax.rem(self.y + o + self.ys, self.ys)

    def first(self, k, back=False):
        out = []
        for o in range(1, self.xs):
            ref = self.buf.at[k, 0:2, self.y, self.east(-o) if back else self.x, self.c]
            out.append(self.move(ref, ref, self.s1a.at[k, o], self.r1a.at[k, o], self.y, self.east(o), self.c))
        for o in range(1, self.ys):
            ref = self.buf.at[k, 2:3, self.north(-o) if back else self.y, self.x, self.c]
            out.append(self.move(ref, ref, self.s1b.at[k, o], self.r1b.at[k, o], self.north(o), self.x, self.c))
        return out

    def second(self, k, back=False):
        out = []
        for o in range(1, self.ys):
            ref = self.buf.at[k, 0:2, self.north(-o) if back else self.y, :, self.c]
            out.append(self.move(ref, ref, self.s2a.at[k, o], self.r2a.at[k, o], self.north(o), self.x, self.c))
        for o in range(1, self.xs):
            ref = self.buf.at[k, 2:3, :, self.east(-o) if back else self.x, self.c]
            out.append(self.move(ref, ref, self.s2b.at[k, o], self.r2b.at[k, o], self.y, self.east(o), self.c))
        return out

    def third(self, k, back=False):
        ref = self.buf.at[k, :, :, :, 1 - self.c if back else self.c]
        return [self.move(ref, ref, self.cs.at[k], self.cr.at[k], self.y, self.x, 1 - self.c)]

    def stage(self, number, k):
        stages = (self.first, self.second, self.third)
        if number > 0:
            for copy in stages[number - 1](k, True):
                copy.wait_recv()
        if number < 3:
            for copy in stages[number](k):
                copy.start()

    def finish(self, k):
        for stage in (self.first, self.second, self.third):
            for copy in stage(k):
                copy.wait_send()

    @staticmethod
    def sems(n_data, count):
        ys, xs = plane(n_data)
        sem = pltpu.SemaphoreType.DMA
        xy = [sem((count, xs)), sem((count, ys))]
        return xy + xy + xy[::-1] + xy[::-1] + [sem((count,)), sem((count,))]


def near_hops(n):
    return min(2, n - 1)


def data_peers(n_data):
    mine = lax.axis_index("dp")
    return [{"dp": lax.rem(mine + off, n_data)} for off in range(1, n_data)]


def front_kernel(
    dims, n_data, x_ref, g_ref, w_ref, gain_ref, c_ref, st_ref,
    n1_ref, q_ref, k_ref, v_ref, lse_ref, oc_ref, wq_out, wt_out, g_near, n2_near, out_ref, dh_ref, n2_ref, dhb_ref, dgain_ref,
    xbuf, wf, wpad, mask, opad, of_ref, h_ref, acc, dn2, zs, zr, ws, wr, gs, gr, ns, nr, as_, ar, os_, *plane_sems,
):
    n, rows, heads, span = dims
    hops_g = near_hops(n)
    me = lax.axis_index("mp")
    cols = w_ref.shape[2]
    width = x_ref.shape[1]
    greet(line_peers(n, me) + data_peers(n_data))
    gather = LineGather(n, me, own_then(x_ref, xbuf), xbuf, zs, zr)
    whole = PlaneGather(n_data, wf, plane_sems)

    def place(k):
        return wf.at[k, :, whole.y, whole.x, whole.c]

    class Weights(LineGather):
        def copy(self, slot, hop, way):
            return pltpu.make_async_remote_copy(
                src_ref=place(slot), dst_ref=place(slot), send_sem=self.ssem.at[way, hop],
                recv_sem=self.rsem.at[slot], device_id={"mp": self.me + 1 - 2 * way}, device_id_type=MESH,
            )

    lines = Weights(n, me, None, None, ws, wr)
    gather_g = LineGather(n, me, own_then(g_ref, g_near), g_near, gs, gr)
    gather_n = LineGather(n, me, own_then(n2_ref, n2_near), n2_near, ns, nr)
    gather.send(0)
    place(n)[...] = w_ref[0:3]
    place(me)[...] = w_ref[3:6]
    whole.stage(0, n)
    lines.send(0)
    whole.stage(0, me)
    sel = spread(cols, heads)
    xbuf[me] = x_ref[...]

    def matrix(k, m):
        value = wf[k, m]
        if value.shape[-2] % 16:
            return value.astype(F32).reshape(width, cols).astype(BF16)
        return value.reshape(width, cols)

    whole.stage(1, n)
    whole.stage(1, me)
    whole.stage(2, n)
    whole.stage(2, me)
    whole.stage(3, n)
    for m in range(3):
        wpad[m] = nn(matrix(n, m), sel).astype(BF16)

    def project(slot):
        x = xbuf[slot].astype(F32)
        scale = lax.rsqrt(jnp.mean(x * x, axis=-1, keepdims=True) + EPSILON)
        normed = (x * scale * gain_ref[0:1]).astype(BF16)
        n1_ref[slot] = normed
        at = block_rows(slot, rows)
        for m, ref in enumerate((q_ref, k_ref, v_ref)):
            out = nn(normed, wpad[m])
            if m == 0:
                out = out * c_ref[...]
            out = out.astype(BF16)
            for h in range(heads):
                ref[h, at, :] = out[:, h * LANE : (h + 1) * LANE]

    project(me)

    def arrivals(hop, do):
        def one(way, _):
            slot = me - hop + 2 * hop * way

            @pl.when((slot >= 0) & (slot < n))
            def _():
                do(slot)

            return 0

        lax.fori_loop(0, 2, one, 0)

    def forward(stage, hop):
        if 1 <= hop < n:
            arrivals(hop, lambda slot: whole.stage(stage, slot))

    for hop in range(1, n):
        gather.relay(hop)
        if hop < n - 1:
            lines.relay(hop)
            forward(0, hop)
        forward(1, hop - 1)
        arrivals(hop, project)
        forward(2, hop - 1)
    gather_g.send(0)

    def chunk(i, _):
        first = jnp.maximum(i - (span - 1), 0)
        at, keys = block_rows(i, rows), pl.ds(pl.multiple_of(first * rows, rows), span * rows)
        q_pos = i * rows + lax.broadcasted_iota(jnp.int32, mask.shape, 0)
        k_pos = first * rows + lax.broadcasted_iota(jnp.int32, mask.shape, 1)
        mask[...] = jnp.where((k_pos <= q_pos) & (k_pos >= st_ref[at, :]), 0.0, NEG)

        def head(h, _):
            scores = nt(q_ref[h, at, :], k_ref[h, keys, :]) + mask[...]
            top = jnp.max(scores, axis=-1, keepdims=True)
            raised = jnp.exp(scores - top)
            total = jnp.sum(raised, axis=-1, keepdims=True)
            prob = (raised * (1.0 / total)).astype(BF16)
            opad[h] = nn(prob, v_ref[h, keys, :]).astype(BF16)
            lse_ref[h, at, :] = top + jnp.log(total)
            return 0

        lax.fori_loop(0, heads, head, 0)
        wide = jnp.concatenate([opad[h] for h in range(heads)], axis=1)
        oc_ref[i] = nt(wide, sel).astype(BF16)

        @pl.when(i != me)
        def _():
            pltpu.make_async_remote_copy(
                src_ref=oc_ref.at[i], dst_ref=of_ref.at[me], send_sem=as_.at[i],
                recv_sem=ar.at[me], device_id={"mp": i}, device_id_type=MESH,
            ).start()

        @pl.when(i == me)
        def _():
            of_ref[me] = oc_ref[me]

        @pl.when(i == 0)
        def _():
            lines.relay(n - 1)
            forward(0, n - 1)

        @pl.when(i == n // 2)
        def _():
            forward(1, n - 1)

        return 0

    lax.fori_loop(0, n, chunk, 0)
    forward(2, n - 1)

    def both(slot, _):
        whole.stage(3, slot)
        return 0

    lax.fori_loop(0, n, both, 0)
    keep_q = pltpu.make_async_copy(wf.at[n], wq_out, os_.at[0])
    keep_t = pltpu.make_async_copy(wf.at[me], wt_out, os_.at[1])
    keep_q.start()
    keep_t.start()
    for hop in range(1, hops_g):
        gather_g.relay(hop)
    h_ref[...] = x_ref[...].astype(F32) + nt(of_ref[me], matrix(me, 0))

    def outward(off, _):
        peer = lax.rem(me + off, n)
        copy = pltpu.make_async_remote_copy(
            src_ref=oc_ref.at[peer], dst_ref=of_ref.at[peer], send_sem=as_.at[peer],
            recv_sem=ar.at[peer], device_id={"mp": peer}, device_id_type=MESH,
        )
        copy.wait_recv()
        h_ref[...] += nt(of_ref[peer], matrix(peer, 0))
        copy.wait_send()
        return 0

    lax.fori_loop(1, n, outward, 0)
    h = h_ref[...]
    scale = lax.rsqrt(jnp.mean(h * h, axis=-1, keepdims=True) + EPSILON)
    n2_ref[...] = (h * scale * gain_ref[1:2]).astype(BF16)
    gather_n.send(0)
    acc[...] = h
    dn2[...] = jnp.zeros_like(dn2)

    def hidden(j, _):
        up, down = matrix(j, 1), matrix(j, 2)
        gate = nn(n2_ref[...], up)
        sig = 1.0 / (1.0 + jnp.exp(-gate))
        acc[...] += nt((gate * sig).astype(BF16), down)
        dz = nn(g_ref[...], down)
        da = (dz * (sig * (1.0 + gate * (1.0 - sig)))).astype(BF16)
        dn2[...] += nt(da, up)
        return 0

    lax.fori_loop(0, n, hidden, 0)
    out_ref[...] = acc[...].astype(BF16)
    h = h_ref[...]
    scale = lax.rsqrt(jnp.mean(h * h, axis=-1, keepdims=True) + EPSILON)
    unit = h * scale
    grad = dn2[...]
    dgain_ref[...] = jnp.sum(grad * unit, axis=0, keepdims=True)
    du = grad * gain_ref[1:2]
    dh = g_ref[...].astype(F32) + scale * (du - unit * jnp.mean(du * unit, axis=-1, keepdims=True))
    dh_ref[...] = dh
    dhb_ref[...] = dh.astype(BF16)
    gather_g.take(hops_g)
    gather_n.take(1)
    gather_g.finish(0, hops_g)
    gather_n.finish(0, 1)
    gather.finish()
    lines.finish()

    def sent(k, _):
        whole.finish(k)
        return 0

    lax.fori_loop(0, n + 1, sent, 0)
    keep_q.wait()
    keep_t.wait()


def front(dims, x, g, shards, gains, c_row, starts):
    n, rows, heads, span = dims
    n_data = lax.axis_size("dp")
    own_rows, cols = shards.shape[1:]
    width = x.shape[1]
    count = n * rows
    ys, xs = plane(n_data)
    head_out = jax.ShapeDtypeStruct((heads, count, LANE), BF16)
    kept = jax.ShapeDtypeStruct((3, ys, xs, 2, own_rows, cols), BF16)
    own = jax.ShapeDtypeStruct((rows, width), BF16)
    sem = pltpu.SemaphoreType.DMA
    return pl.pallas_call(
        functools.partial(front_kernel, dims, n_data),
        out_shape=(
            jax.ShapeDtypeStruct((n, rows, width), BF16),
            head_out, head_out, head_out,
            jax.ShapeDtypeStruct((heads, count, 1), F32),
            jax.ShapeDtypeStruct((n, rows, cols), BF16),
            kept, kept,
            jax.ShapeDtypeStruct((n, rows, width), BF16),
            jax.ShapeDtypeStruct((n, rows, width), BF16),
            own,
            jax.ShapeDtypeStruct((rows, width), F32),
            own, own,
            jax.ShapeDtypeStruct((1, width), F32),
        ),
        in_specs=vmem(6),
        out_specs=vmem(6) + [pl.BlockSpec(memory_space=pl.ANY)] * 4 + vmem(5),
        scratch_shapes=[
            pltpu.VMEM((n, rows, width), BF16),
            pltpu.VMEM((n + 1, *kept.shape), BF16),
            pltpu.VMEM((3, width, heads * LANE), BF16),
            pltpu.VMEM((rows, span * rows), F32),
            pltpu.VMEM((heads, rows, LANE), BF16),
            pltpu.VMEM((n, rows, cols), BF16),
            pltpu.VMEM((rows, width), F32), pltpu.VMEM((rows, width), F32), pltpu.VMEM((rows, width), F32),
            *line_sems(n), *line_sems(n), *line_sems(n), *line_sems(n),
            sem((n,)), sem((n,)), sem((2,)),
            *PlaneGather.sems(n_data, n + 1),
        ],
        compiler_params=params(1),
        name="front",
    )(x, g, shards, gains, c_row, starts)


def back_kernel(
    dims, q_ref, k_ref, v_ref, lse_ref, own_ref, c_ref, st_ref, w_hbm,
    dx_ref, dc_ref, dhb_ref,
    w_ref, wpad, mask, do_ref, dq_ref, dk_ref, dv_ref, zs, zr, w_sem,
):
    n, rows, heads, span = dims
    me = lax.axis_index("mp")
    take_w = pltpu.make_async_copy(w_hbm.at[0], w_ref, w_sem)
    take_w.start()
    greet(line_peers(n, me))
    gather = LineGather(n, me, own_then(own_ref, dhb_ref), dhb_ref, zs, zr)
    gather.send(0)
    dhb_ref[me] = own_ref[...]
    sel = spread(w_ref.shape[1], heads)
    take_w.wait()
    wpad[...] = nn(w_ref[...], sel).astype(BF16)
    dk_ref[...] = jnp.zeros_like(dk_ref)
    dv_ref[...] = jnp.zeros_like(dv_ref)
    dc_ref[...] = jnp.zeros_like(dc_ref)

    def squeeze(ref, at):
        wide = jnp.concatenate([ref[h, at, :].astype(BF16) for h in range(heads)], axis=1)
        return nt(wide, sel).astype(BF16)

    def chunk(i):
        first = jnp.maximum(i - (span - 1), 0)
        at, keys = block_rows(i, rows), pl.ds(pl.multiple_of(first * rows, rows), span * rows)
        q_pos = i * rows + lax.broadcasted_iota(jnp.int32, mask.shape, 0)
        k_pos = first * rows + lax.broadcasted_iota(jnp.int32, mask.shape, 1)
        mask[...] = jnp.where((k_pos <= q_pos) & (k_pos >= st_ref[at, :]), 0.0, NEG)
        grad = nn(dhb_ref[i], wpad[...]).astype(BF16)
        for h in range(heads):
            do_ref[h] = grad[:, h * LANE : (h + 1) * LANE]

        def head(h, _):
            query = q_ref[h, at, :]
            scores = nt(query, k_ref[h, keys, :]) + mask[...]
            prob = jnp.exp(scores - lse_ref[h, at, :])
            dp = nt(do_ref[h], v_ref[h, keys, :])
            inner = jnp.sum(prob * dp, axis=-1, keepdims=True)
            ds = (prob * (dp - inner)).astype(BF16)
            dq = nn(ds, k_ref[h, keys, :])
            dk_ref[h, keys, :] += tn(ds, query)
            dv_ref[h, keys, :] += tn(prob.astype(BF16), do_ref[h])
            dc_ref[...] += jnp.sum(dq * query.astype(F32), axis=0, keepdims=True)
            dq_ref[h] = (dq * c_ref[:, :LANE]).astype(BF16)
            return 0

        lax.fori_loop(0, heads, head, 0)
        dx_ref[0, i] = squeeze(dq_ref, slice(None))

    def event(e, _):
        hop, way = (e + 1) // 2, lax.rem(e + 1, 2)
        i = me - hop + 2 * hop * way

        @pl.when((way == 0) & (hop > 0))
        def _():
            for fixed in range(1, n):

                @pl.when(hop == fixed)
                def _(fixed=fixed):
                    gather.relay(fixed)

        @pl.when((i >= 0) & (i < n))
        def _():
            chunk(i)

        return 0

    lax.fori_loop(0, 2 * n - 1, event, 0)

    def close(i, _):
        at = block_rows(i, rows)
        dx_ref[1, i] = squeeze(dk_ref, at)
        dx_ref[2, i] = squeeze(dv_ref, at)
        return 0

    lax.fori_loop(0, n, close, 0)
    gather.finish()


def back(dims, q, k, v, lse, dhb, c_row, starts, w_tail):
    n, rows, heads, span = dims
    width, cols = w_tail.shape[1:]
    return pl.pallas_call(
        functools.partial(back_kernel, dims),
        out_shape=(
            jax.ShapeDtypeStruct((3, n, rows, cols), BF16),
            jax.ShapeDtypeStruct((1, LANE), F32),
            jax.ShapeDtypeStruct((n, rows, width), BF16),
        ),
        in_specs=vmem(7) + [pl.BlockSpec(memory_space=pl.ANY)],
        out_specs=vmem(3),
        scratch_shapes=[
            pltpu.VMEM((width, cols), BF16),
            pltpu.VMEM((width, heads * LANE), BF16),
            pltpu.VMEM((rows, span * rows), F32),
            pltpu.VMEM((heads, rows, LANE), BF16),
            pltpu.VMEM((heads, rows, LANE), BF16),
            pltpu.VMEM((heads, n * rows, LANE), F32),
            pltpu.VMEM((heads, n * rows, LANE), F32),
            *line_sems(n),
            pltpu.SemaphoreType.DMA,
        ],
        compiler_params=params(2),
        name="back",
    )(q, k, v, lse, dhb, c_row, starts, w_tail)


def halves(value):
    high = value.astype(BF16)
    return high, (value - high.astype(F32)).astype(BF16)


def dot_split(small, big, contract):
    count = small.shape[0]
    high, low = halves(small)
    big_high, big_low = halves(big)
    both = contract(jnp.concatenate([high.astype(F32), low.astype(F32)], axis=0).astype(BF16), big_high)
    return both[:count] + both[count:] + contract(high, big_low)


class PlaneScatter:
    def __init__(self, n_data, gb, core, a1, b1, a2, b2, sems):
        self.ys, self.xs = plane(n_data)
        self.gb, self.core, self.a1, self.b1, self.a2, self.b2 = gb, core, a1, b1, a2, b2
        (self.c_s, self.c_r, self.s1, self.ra1, self.rb1, self.s2, self.ra2, self.rb2) = sems
        me = lax.axis_index("dp")
        self.c = lax.rem(me, 2)
        self.x = lax.rem(me // 2, self.xs)
        self.y = me // (2 * self.xs)
        self.half = gb.shape[0] // 2

    def send(self, src, dst, ssem, rsem, y, x, c):
        return pltpu.make_async_remote_copy(
            src_ref=src, dst_ref=dst, send_sem=ssem, recv_sem=rsem,
            device_id={"dp": (y * self.xs + x) * 2 + c}, device_id_type=MESH,
        )

    def copies_core(self):
        other = 1 - self.c
        src = self.gb.at[:, :, :, other]
        return [self.send(src, self.core, self.c_s, self.c_r, self.y, self.x, other)]

    def copies_one(self):
        out, h = [], self.half
        for o in range(1, self.xs):
            to = lax.rem(self.x + o, self.xs)
            src = self.core.at[:h, :, to]
            out.append(self.send(src, self.a1.at[o - 1], self.s1.at[0, o], self.ra1.at[o], self.y, to, self.c))
        for o in range(1, self.ys):
            to = lax.rem(self.y + o, self.ys)
            src = self.core.at[h:, to]
            out.append(self.send(src, self.b1.at[o - 1], self.s1.at[1, o], self.rb1.at[o], to, self.x, self.c))
        return out

    def copies_two(self):
        out, h = [], self.half
        for o in range(1, self.ys):
            to = lax.rem(self.y + o, self.ys)
            src = self.core.at[:h, to, self.x]
            out.append(self.send(src, self.a2.at[o - 1], self.s2.at[0, o], self.ra2.at[o], to, self.x, self.c))
        for o in range(1, self.xs):
            to = lax.rem(self.x + o, self.xs)
            src = self.core.at[h:, self.y, to]
            out.append(self.send(src, self.b2.at[o - 1], self.s2.at[1, o], self.rb2.at[o], self.y, to, self.c))
        return out

    def start(self, copies):
        for copy in copies:
            copy.start()

    def arrive(self, copies):
        for copy in copies:
            copy.wait_recv()

    def sum_core(self):
        self.arrive(self.copies_core())

        def one(i, _):
            m, rest = i // (self.ys * self.xs), lax.rem(i, self.ys * self.xs)
            y, x = rest // self.xs, lax.rem(rest, self.xs)
            total = self.core[m, y, x].astype(F32) + self.gb[m, y, x, self.c].astype(F32)
            self.core[m, y, x] = total.astype(BF16)
            return 0

        lax.fori_loop(0, self.gb.shape[0] * self.ys * self.xs, one, 0)

    def sum_one(self):
        self.arrive(self.copies_one())
        h = self.half

        def along_y(i, _):
            m, y = i // self.ys, lax.rem(i, self.ys)
            total = self.core[m, y, self.x].astype(F32)
            for o in range(1, self.xs):
                total += self.a1[o - 1, m, y].astype(F32)
            self.core[m, y, self.x] = total.astype(BF16)
            return 0

        def along_x(i, _):
            m, x = i // self.xs, lax.rem(i, self.xs)
            total = self.core[h + m, self.y, x].astype(F32)
            for o in range(1, self.ys):
                total += self.b1[o - 1, m, x].astype(F32)
            self.core[h + m, self.y, x] = total.astype(BF16)
            return 0

        lax.fori_loop(0, h * self.ys, along_y, 0)
        lax.fori_loop(0, h * self.xs, along_x, 0)

    def sum_two(self, put):
        self.arrive(self.copies_two())
        for m in range(self.half):
            total = self.core[m, self.y, self.x].astype(F32)
            for o in range(1, self.ys):
                total += self.a2[o - 1, m].astype(F32)
            put(m, total)
            total = self.core[self.half + m, self.y, self.x].astype(F32)
            for o in range(1, self.xs):
                total += self.b2[o - 1, m].astype(F32)
            put(self.half + m, total)

    def finish(self):
        for copy in self.copies_core() + self.copies_one() + self.copies_two():
            copy.wait_send()

    @staticmethod
    def scratch(n_data, count, rows, cols):
        ys, xs = plane(n_data)
        h = count // 2
        sem = pltpu.SemaphoreType.DMA
        return [
            pltpu.VMEM((count, ys, xs, 2, rows, cols), BF16),
            pltpu.VMEM((count, ys, xs, rows, cols), BF16),
            pltpu.VMEM((max(xs - 1, 1), h, ys, rows, cols), BF16),
            pltpu.VMEM((max(ys - 1, 1), h, xs, rows, cols), BF16),
            pltpu.VMEM((max(ys - 1, 1), h, rows, cols), BF16),
            pltpu.VMEM((max(xs - 1, 1), h, rows, cols), BF16),
            sem, sem, sem((2, max(xs, ys))), sem((xs,)), sem((ys,)),
            sem((2, max(xs, ys))), sem((ys,)), sem((xs,)),
        ]


class Exchange:
    def __init__(self, axis, size, src_of, dst, ssem, rsem):
        self.axis, self.size, self.src_of, self.dst, self.ssem, self.rsem = axis, size, src_of, dst, ssem, rsem
        self.me = lax.axis_index(axis)

    def copy(self, peer, slot):
        return pltpu.make_async_remote_copy(
            src_ref=self.src_of(peer), dst_ref=self.dst.at[slot], send_sem=self.ssem.at[peer],
            recv_sem=self.rsem.at[slot], device_id={self.axis: peer}, device_id_type=MESH,
        )

    def each(self, do):
        def one(off, _):
            do(lax.rem(self.me + off, self.size))
            return 0

        lax.fori_loop(1, self.size, one, 0)

    def start(self):
        self.each(lambda peer: self.copy(peer, self.me).start())

    def arrive(self):
        self.each(lambda peer: self.copy(peer, peer).wait_recv())

    def finish(self):
        self.each(lambda peer: self.copy(peer, peer).wait_send())


def total_of(ref, size):
    def one(i, total):
        return total + ref[i]

    return lax.fori_loop(1, size, one, ref[0])


FIRST, SECOND = (0, 1, 2, 4), (3, 5)


class Factors:
    def __init__(self, n, n_data, group, index, ft, m_ref, basis, right, refs):
        self.group, self.index, self.ft, self.m, self.basis, self.right = group, index, ft, m_ref, basis, right
        self.send, self.got, self.line, self.full, self.rgot = refs[:5]
        l_s, l_r, z_s, z_r, a_s, a_r, r_s, r_r = refs[5:]
        self.n, self.n_data = n, n_data
        self.tiles = basis.shape[2] // LANE
        self.per = self.send.shape[1]
        self.mine, self.me = lax.axis_index("dp"), lax.axis_index("mp")
        mine, me = self.mine, self.me
        self.ex_left = Exchange("dp", n_data, lambda peer: self.send.at[peer], self.got, l_s, l_r)
        self.ex_line = Exchange("mp", n, lambda peer: self.line.at[me], self.line, z_s, z_r)
        self.ex_all = Exchange("dp", n_data, lambda peer: self.full.at[mine], self.full, a_s, a_r)
        self.ex_right = Exchange("dp", n_data, lambda peer: self.rgot.at[mine], self.rgot, r_s, r_r)

    def start(self):
        size = len(self.group) * self.tiles
        for tile in range(size, self.n_data * self.per):
            self.send[tile // self.per, tile % self.per] = jnp.zeros((8, LANE), F32)

        def rows_of(k, _):
            m = self.index(k)
            rows_left = dot_split(self.ft[m], self.m[m], nn)
            for t in range(self.tiles):
                tile = k * self.tiles + t
                self.send[tile // self.per, lax.rem(tile, self.per)] = rows_left[:, t * LANE : (t + 1) * LANE]
            return 0

        lax.fori_loop(0, len(self.group), rows_of, 0)
        self.got[self.mine] = self.send[self.mine]
        self.ex_left.start()

    def along_line(self):
        self.ex_left.arrive()
        self.line[self.me] = total_of(self.got, self.n_data)
        self.ex_line.start()

    def spread_out(self):
        self.ex_line.arrive()
        self.full[self.mine] = total_of(self.line, self.n)
        self.ex_all.start()

    def orthonormal(self):
        self.ex_all.arrive()
        tiles, per = self.tiles, self.per
        basis = jnp.stack(
            [
                jnp.concatenate([self.full[t // per, t % per] for t in range(k * tiles, (k + 1) * tiles)], axis=1)
                for k in range(len(self.group))
            ]
        )
        row = lax.broadcasted_iota(jnp.int32, (1, 8, 1), 1)
        for index in range(8):
            vector = basis[:, index : index + 1, :]
            vector = vector * lax.rsqrt(jnp.sum(vector * vector, axis=-1, keepdims=True) + 1e-12)
            onto = jnp.where(row > index, jnp.sum(basis * vector, axis=-1, keepdims=True), 0.0)
            basis = jnp.where(row == index, vector, basis - onto * vector)
        for k, m in enumerate(self.group):
            self.basis[m] = basis[k]

        def rows_of(k, _):
            m = self.index(k)
            self.rgot[self.mine, k] = dot_split(self.basis[m], self.m[m], nt)
            return 0

        lax.fori_loop(0, len(self.group), rows_of, 0)
        self.ex_right.start()

    def close(self):
        self.ex_right.arrive()
        total = total_of(self.rgot, self.n_data)
        for k, m in enumerate(self.group):
            self.right[m] = total[k]

    def finish(self):
        for exchange in (self.ex_left, self.ex_line, self.ex_all, self.ex_right):
            exchange.finish()

    @staticmethod
    def scratch(n, n_data, count, width, cols):
        sem = pltpu.SemaphoreType.DMA
        per = -(-(count * width // LANE) // n_data)
        tiles = (per, 8, LANE)
        return [
            pltpu.VMEM((n_data, *tiles), F32), pltpu.VMEM((n_data, *tiles), F32),
            pltpu.VMEM((n, *tiles), F32), pltpu.VMEM((n_data, *tiles), F32),
            pltpu.VMEM((n_data, count, 8, cols), F32),
            sem((n_data,)), sem((n_data,)), sem((n,)), sem((n,)),
            sem((n_data,)), sem((n_data,)), sem((n_data,)), sem((n_data,)),
        ]


def grads_kernel(
    dims, n_data, scaling, n1_ref, n2_ref, n2_near, dhb_ref, g_ref, g_near, dx_hbm, oc_hbm, wqkv_hbm, wtail_hbm,
    err_ref, x_ref, dh_ref, gain_ref, dgain2_ref, dscale_ref, ft_ref,
    gin_sum, gout_sum, gin_ref, basis_ref, right_ref, small_ref, m_out, n2_far, g_far,
    abuf, dx_ref, wbuf, sbuf, lbuf, m_ref, srecv, szrecv,
    fs, ns_, nr_, gs_, gr_, gts, gtr, nts, ntr, ss, ls, es, ms, g_s, g_r, gz_s, gz_r, *refs,
):
    n, rows, heads, span = dims
    hops_g = near_hops(n)
    me, mine = lax.axis_index("mp"), lax.axis_index("dp")
    width, cols = wbuf.shape[1:]
    tiles = width // LANE
    sizes = (14, 14, 13, 13)
    cuts = [sum(sizes[:k]) for k in range(5)]
    parts = [refs[cuts[k] : cuts[k + 1]] for k in range(4)]

    def load(m):
        return pltpu.make_async_copy(err_ref.at[m], m_ref.at[m], es.at[m])

    def save(m):
        return pltpu.make_async_copy(m_ref.at[m], m_out.at[m], ms.at[m])

    take_dx = pltpu.make_async_copy(dx_hbm, dx_ref, fs.at[0])
    take_oc = pltpu.make_async_copy(oc_hbm, dx_ref.at[2], fs.at[1])
    take_qkv = pltpu.make_async_copy(wqkv_hbm, wbuf, fs.at[2])
    take_tail = pltpu.make_async_copy(wtail_hbm, wbuf, fs.at[3])
    take_dhb = pltpu.make_async_copy(dhb_ref, abuf.at[0], fs.at[4])
    take_n1 = pltpu.make_async_copy(n1_ref, abuf.at[1], fs.at[5])
    take_dx.start()
    take_qkv.start()
    take_n1.start()
    for m in range(6):
        load(m).start()
    take_dhb.start()
    greet(line_peers(n, me) + data_peers(n_data))
    scatter_1 = PlaneScatter(n_data, *parts[0][:6], parts[0][6:])
    scatter_2 = PlaneScatter(n_data, *parts[1][:6], parts[1][6:])
    chain_1 = Factors(n, n_data, FIRST, lambda k: k + k // 3, ft_ref, m_ref, basis_ref, right_ref, parts[2])
    chain_2 = Factors(n, n_data, SECOND, lambda k: 3 + 2 * k, ft_ref, m_ref, basis_ref, right_ref, parts[3])
    gb_1, gb_2 = parts[0][0], parts[1][0]
    ex_small = Exchange("dp", n_data, lambda peer: srecv.at[mine], srecv, g_s, g_r)
    ex_small_line = Exchange("mp", n, lambda peer: szrecv.at[me], szrecv, gz_s, gz_r)

    def follow(own, near, far, hops):
        def source(hop, slot):
            return own if hop == 0 else near.at[slot] if hop <= hops else far.at[slot]

        return source

    gather_n = LineGather(n, me, follow(n2_ref, n2_near, n2_far, 1), n2_far, nts, ntr)
    gather_g = LineGather(n, me, follow(g_ref, g_near, g_far, hops_g), g_far, gts, gtr)

    def bring(step):
        for gather, hops in ((gather_g, hops_g), (gather_n, 1)):
            hop = hops + step
            if step == 0 and hop < n - 1:
                gather.send(hop)
            elif step > 0 and hop <= n - 1:
                gather.relay(hop)

    bring(0)

    def pieces(own, near, far, hops, slot_of, sems, do):
        for i in range(n):
            away = jnp.maximum(i - me, me - i)
            for src, hit in ((own, away == 0), (near.at[i], (away >= 1) & (away <= hops)), (far.at[i], away > hops)):

                @pl.when(hit)
                def _(src=src, i=i):
                    do(pltpu.make_async_copy(src, abuf.at[slot_of, i], sems.at[i]))

    def take_inputs(do):
        pieces(n2_ref, n2_near, n2_far, 1, 0, ns_, do)
        pieces(g_ref, g_near, g_far, hops_g, 1, gs_, do)


    def own(e, _):
        i = jnp.where(lax.rem(e, 2) == 0, n - 1 - e // 2, e // 2)
        total = nt(dx_ref[0, i], wbuf[0])
        total += nt(dx_ref[1, i], wbuf[1])
        total += nt(dx_ref[2, i], wbuf[2])

        @pl.when(i == me)
        def _():
            gin_ref[...] = total

        @pl.when(i != me)
        def _():
            sbuf[i] = total.astype(BF16)

        return 0

    take_dx.wait()
    take_qkv.wait()
    lax.fori_loop(0, n, own, 0)
    take_tail.start()

    def copy(i, way, here=False):
        slot = i if way == 0 else jnp.where(i == (me if here else me - 1), n, i)
        return pltpu.make_async_remote_copy(
            src_ref=sbuf.at[i], dst_ref=lbuf.at[slot], send_sem=ss.at[i], recv_sem=ls.at[slot],
            device_id={"mp": me + 1 - 2 * way}, device_id_type=MESH,
        )

    def launch():
        @pl.when(me == 0)
        def _():
            for i in range(n - 1, 0, -1):
                copy(i, 0).start()

        @pl.when(me == n - 1)
        def _():
            for i in range(n - 1):
                copy(i, 1).start()

    def relay(r):
        for way in (0, 1):
            place = me if way == 0 else n - 1 - me
            i = n - 1 - r + me if way == 0 else r - (n - 1 - me)

            @pl.when((place >= 1) & (place <= r))
            def _(i=i, way=way):
                copy(i, way, True).wait_recv()
                sbuf[i] = (sbuf[i].astype(F32) + lbuf[i].astype(F32)).astype(BF16)
                copy(i, way).start()

    launch()

    def hidden(i, _):
        gate = nn(abuf[0, i], wbuf[1])
        sig = 1.0 / (1.0 + jnp.exp(-gate))
        dx_ref[0, i] = (gate * sig).astype(BF16)
        dz = nn(abuf[1, i], wbuf[2])
        dx_ref[1, i] = (dz * (sig * (1.0 + gate * (1.0 - sig)))).astype(BF16)
        return 0

    def flat(value):
        return value.reshape(n * rows, value.shape[-1])

    def weight(m, gb, k, a, b):
        left, right = flat(a), flat(b)
        load(m).wait()
        m_ref[m] = scaling * tn(right, left) + m_ref[m]
        gb[k] = tn(left, right).reshape(gb.shape[1:]).astype(BF16)

    def inputs(m, _):
        weight(m, gb_1, m, abuf[1], dx_ref[m])
        return 0

    take_n1.wait()
    lax.fori_loop(0, 3, inputs, 0)
    take_oc.start()
    bring(1)
    take_dhb.wait()
    take_oc.wait()
    weight(4, gb_1, 3, abuf[0], dx_ref[2])
    chain_1.start()
    scatter_1.start(scatter_1.copies_core())
    relay(1)
    chain_1.along_line()
    scatter_1.sum_core()
    scatter_1.start(scatter_1.copies_one())
    chain_1.spread_out()
    chain_1.orthonormal()
    for r in range(2, n - 1):
        relay(r)
        bring(r)
    bring(n - 1)
    take_inputs(lambda c: c.start())
    scatter_1.sum_one()
    scatter_1.start(scatter_1.copies_two())
    take_tail.wait()
    take_inputs(lambda c: c.wait())
    lax.fori_loop(0, n, hidden, 0)

    def late(k, _):
        weight(3 + 2 * k, gb_2, k, abuf[k], dx_ref[1 - k])
        return 0

    lax.fori_loop(0, 2, late, 0)
    chain_2.start()
    scatter_2.start(scatter_2.copies_core())
    for m in range(6):
        save(m).start()


    @pl.when(me > 0)
    def _():
        copy(me, 0).wait_recv()
        gin_ref[...] += lbuf[me].astype(F32)

    @pl.when(me < n - 1)
    def _():
        copy(me, 1, True).wait_recv()
        gin_ref[...] += lbuf[n].astype(F32)

    chain_2.along_line()
    x = x_ref[...].astype(F32)
    scale = lax.rsqrt(jnp.mean(x * x, axis=-1, keepdims=True) + EPSILON)
    unit = x * scale
    grad = gin_ref[...]
    dgain = jnp.sum(grad * unit, axis=0, keepdims=True)
    srecv[mine] = jnp.zeros(srecv.shape[1:], F32)
    for t in range(tiles):
        at = slice(t * LANE, (t + 1) * LANE)
        srecv[mine, t // 8, t % 8 : t % 8 + 1, :] = scaling * dgain[:, at]
        t2 = tiles + t
        srecv[mine, t2 // 8, t2 % 8 : t2 % 8 + 1, :] = scaling * dgain2_ref[:, at]
    t3 = 2 * tiles
    srecv[mine, t3 // 8, t3 % 8 : t3 % 8 + 1, :] = scaling * dscale_ref[...]
    ex_small.start()
    scatter_2.sum_core()
    scatter_2.start(scatter_2.copies_one())
    chain_2.spread_out()
    du = grad * gain_ref[...]
    gin_ref[...] = dh_ref[...] + scale * (du - unit * jnp.mean(du * unit, axis=-1, keepdims=True))
    ex_small.arrive()
    szrecv[me] = total_of(srecv, n_data)
    ex_small_line.start()
    chain_2.orthonormal()

    def put_1(k, value):
        if k < 3:
            gin_sum[k] = scaling * value
        else:
            gout_sum[0] = scaling * value

    def put_2(k, value):
        (gout_sum if k else gin_sum)[1 if k else 3] = scaling * value

    scatter_1.sum_two(put_1)
    chain_1.close()
    scatter_2.sum_one()
    scatter_2.start(scatter_2.copies_two())
    ex_small_line.arrive()
    small_ref[...] = total_of(szrecv, n)
    chain_2.close()
    scatter_2.sum_two(put_2)

    for i in range(n):

        @pl.when(me < i)
        def _(i=i):
            copy(i, 0).wait_send()

        @pl.when(me > i)
        def _(i=i):
            copy(i, 1).wait_send()

    chain_1.finish()
    chain_2.finish()
    ex_small.finish()
    ex_small_line.finish()
    scatter_1.finish()
    scatter_2.finish()
    gather_g.finish(hops_g)
    gather_n.finish(1)
    for m in range(6):
        save(m).wait()


def grads(dims, scaling, hbm, x, dh, gain, dgain2, dscale, ft):
    n, rows = dims[:2]
    n_data = lax.axis_size("dp")
    width, cols = hbm[-2].shape[1:]
    own_rows = width // n_data
    sem = pltpu.SemaphoreType.DMA
    small = -(-(2 * width // LANE + 1) // 8)
    far = jax.ShapeDtypeStruct((n, rows, width), BF16)

    def f32(*shape):
        return pltpu.VMEM(shape, F32)

    def out(*shape):
        return jax.ShapeDtypeStruct(shape, F32)

    return pl.pallas_call(
        functools.partial(grads_kernel, dims, n_data, scaling),
        out_shape=(
            out(4, own_rows, cols), out(2, own_rows, cols), out(rows, width),
            out(6, 8, width), out(6, 8, cols), out(small, 8, LANE),
            out(6, cols, width), far, far,
        ),
        in_specs=[pl.BlockSpec(memory_space=pl.ANY)] * len(hbm) + vmem(6),
        out_specs=vmem(6) + [pl.BlockSpec(memory_space=pl.ANY)] * 3,
        scratch_shapes=[
            pltpu.VMEM((2, n, rows, width), BF16),
            pltpu.VMEM((3, n, rows, cols), BF16),
            pltpu.VMEM((3, width, cols), BF16),
            pltpu.VMEM((n, rows, width), BF16),
            pltpu.VMEM((n + 1, rows, width), BF16),
            f32(6, cols, width),
            f32(n_data, small, 8, LANE), f32(n, small, 8, LANE),
            sem((6,)), sem((n,)), sem((n,)), sem((n,)), sem((n,)),
            *line_sems(n), *line_sems(n), sem((n,)), sem((n + 1,)), sem((6,)), sem((6,)),
            sem((n_data,)), sem((n_data,)), sem((n,)), sem((n,)),
            *PlaneScatter.scratch(n_data, 4, own_rows, cols),
            *PlaneScatter.scratch(n_data, 2, own_rows, cols),
            *Factors.scratch(n, n_data, 4, width, cols),
            *Factors.scratch(n, n_data, 2, width, cols),
        ],
        compiler_params=params(3),
        name="grads",
    )(*hbm, x, dh, gain, dgain2, dscale, ft)[:7]


def close_kernel(m_ref, right_ref, basis_ref, out_ref):
    right, basis = right_ref[0], basis_ref[0]
    (rh, rl), (bh, bl) = halves(right), halves(basis)
    left = jnp.concatenate([rh, rl, rh], axis=0)
    out_ref[0] = m_ref[0] - tn(left, jnp.concatenate([bh, bh, bl], axis=0))


def close(m, right, basis):
    cols, width = m.shape[1:]

    def spec(*shape):
        return pl.BlockSpec((1, *shape), lambda i: (i, 0, 0))

    return pl.pallas_call(
        close_kernel,
        grid=(6,),
        out_shape=jax.ShapeDtypeStruct(m.shape, F32),
        in_specs=[spec(cols, width), spec(8, cols), spec(8, width)],
        out_specs=spec(cols, width),
        compiler_params=params(),
        name="close",
    )(m, right, basis)


def on_device(
    activations, cotangent, doc_lengths, w_in, w_attn_out, w_down, gains, scale_param,
    mom_in, mom_out, mom_gain, mom_scale, error_buffer, factors,
):
    rows, width = activations.shape
    n = lax.axis_size("mp")
    data_par = lax.axis_size("dp")
    my_data = lax.axis_index("dp")
    count = rows * n
    scaling = (count * data_par) ** (-0.5)
    cols = w_in.shape[2]
    own_rows = w_in.shape[1]
    heads = cols // HD
    longest = count // 2
    span = min(n, -(-(longest - 1) // rows) + 1)
    dims = (n, rows, heads, span)

    shards = jnp.concatenate([w_in[:3], w_attn_out.T[None], w_in[3:], w_down.T[None]], axis=0).astype(BF16)
    ends = jnp.cumsum(doc_lengths[0])
    position = jnp.arange(count, dtype=jnp.int32)[:, None]
    starts = jnp.max(jnp.where(ends[None, :] <= position, ends[None, :], 0), axis=1, keepdims=True)
    factor = SCALE_BASE / math.sqrt(HD) * jax.nn.softplus(scale_param)
    c_row = jnp.tile(jnp.pad(factor, (0, LANE - HD)), heads)[None]

    n1, q, k, v, lse, oc, wqkv, w_tail, g_near, n2_near, output, dh, n2, dhb, dgain2 = front(
        dims, activations, cotangent, shards, gains, c_row, starts
    )
    wqkv, w_tail = wqkv.reshape(3, width, cols), w_tail.reshape(3, width, cols)
    dx, dc, dhb = back(dims, q, k, v, lse, dhb, c_row, starts, w_tail)
    grad_scale_local = dc[0, :HD] / factor * (SCALE_BASE / math.sqrt(HD)) * jax.nn.sigmoid(scale_param)
    dscale = jnp.pad(grad_scale_local, (0, LANE - HD))[None]
    hbm = (n1, n2, n2_near, dhb, cotangent, g_near, dx, oc, wqkv, w_tail, error_buffer[0])
    grad_in, out_sum, grad_input, basis, right, small, stored = grads(
        dims, scaling, hbm, activations, dh, gains[:1], dgain2, dscale, jnp.swapaxes(factors, 1, 2)
    )
    grad_out = jnp.swapaxes(out_sum, 1, 2)
    error_new = close(stored, right, basis)[None]
    tiles = width // LANE
    small = small.reshape(-1, LANE)
    grad_gain = small[: 2 * tiles].reshape(2, width)
    grad_scale = small[2 * tiles, :HD]
    mine_basis = lax.dynamic_slice_in_dim(basis, my_data * own_rows, own_rows, 2)
    mine = jnp.einsum("krd,krc->kdc", mine_basis, right, precision=HIGHEST)
    right = jnp.swapaxes(right, 1, 2)
    mom_in_new = MOMENTUM * mom_in + mine[:4]
    new_in = w_in - RATE * mom_in_new
    mom_out_new = MOMENTUM * mom_out + jnp.swapaxes(mine[4:], 1, 2)
    new_out = jnp.stack([w_attn_out, w_down]) - RATE * mom_out_new
    mom_gain_new = MOMENTUM * mom_gain + grad_gain
    new_gain = gains - RATE * mom_gain_new
    mom_scale_new = MOMENTUM * mom_scale + grad_scale
    new_scale = scale_param - RATE * mom_scale_new
    return (
        output, grad_input, grad_in, grad_out, grad_gain, grad_scale, new_in, new_out,
        new_gain, new_scale, mom_in_new, mom_out_new, mom_gain_new, mom_scale_new,
        error_new, right,
    )


def solution(mesh):
    tokens, shard = P(("dp", "mp"), None), P(None, "dp", "mp")
    return jax.shard_map(
        on_device,
        mesh=mesh,
        in_specs=(
            tokens, tokens, P("dp", None), shard, P("mp", "dp"), P("mp", "dp"), P(), P(),
            shard, P(None, "mp", "dp"), P(), P(), P("dp", None, "mp", None), P(None, "mp", None),
        ),
        out_specs=(
            tokens, tokens, shard, P(None, "mp", "dp"), P(), P(), shard, P(None, "mp", "dp"),
            P(), P(), shard, P(None, "mp", "dp"), P(), P(), P("dp", None, "mp", None),
            P(None, "mp", None),
        ),
        check_vma=False,
    )
```

```python
import functools
import math

import jax
import jax.numpy as jnp
from jax import lax
from jax.experimental import pallas as pl
from jax.experimental.pallas import tpu as pltpu
from jax.sharding import PartitionSpec as P

HD = 80
LANE = 128
HIGHEST = lax.Precision.HIGHEST
EPSILON = 1e-06
SCALE_BASE = 1.442695041
MOMENTUM = 0.9
RATE = 0.1
NEG = -1e30
F32 = jnp.float32
BF16 = jnp.bfloat16
MESH = pl.DeviceIdType.MESH
VMEM_LIMIT = 67_000_000


def nn(a, b):
    return jnp.dot(a, b, preferred_element_type=F32)


def nt(a, b):
    return lax.dot_general(a, b, (((1,), (1,)), ((), ())), preferred_element_type=F32)


def tn(a, b):
    return lax.dot_general(a, b, (((0,), (0,)), ((), ())), preferred_element_type=F32)


def spread(cols, heads):
    row = lax.broadcasted_iota(jnp.int32, (cols, heads * LANE), 0)
    col = lax.broadcasted_iota(jnp.int32, (cols, heads * LANE), 1)
    off = col & (LANE - 1)
    hit = (row == (col >> 7) * HD + off) & (off < HD)
    return jnp.where(hit, 1.0, 0.0).astype(BF16)


def block_rows(index, rows):
    return pl.ds(pl.multiple_of(index * rows, rows), rows)


def greet(peers):
    bar = pltpu.get_barrier_semaphore()
    for peer in peers:
        pl.semaphore_signal(bar, 1, device_id=peer, device_id_type=MESH)
    pl.semaphore_wait(bar, len(peers))


def line_peers(n, me):
    return [{"mp": lax.rem(me + off, n)} for off in range(1, n)]


class LineGather:
    def __init__(self, n, me, source, buf, ssem, rsem):
        self.n, self.me, self.source, self.buf = n, me, source, buf
        self.ssem, self.rsem = ssem, rsem

    def copy(self, slot, hop, way):
        return pltpu.make_async_remote_copy(
            src_ref=self.source(hop, slot),
            dst_ref=self.buf.at[slot],
            send_sem=self.ssem.at[way, hop],
            recv_sem=self.rsem.at[slot],
            device_id={"mp": self.me + 1 - 2 * way},
            device_id_type=MESH,
        )

    def goes(self, hop, way):
        if way == 0:
            return (self.me - hop >= 0) & (self.me < self.n - 1)
        return (self.me + hop <= self.n - 1) & (self.me > 0)

    def slot(self, hop, way):
        return self.me - hop if way == 0 else self.me + hop

    def arrives(self, hop, way):
        return self.me - hop >= 0 if way == 0 else self.me + hop <= self.n - 1

    def send(self, hop, ways=(0, 1)):
        for way in ways:

            @pl.when(self.goes(hop, way))
            def _(way=way):
                self.copy(self.slot(hop, way), hop, way).start()

    def send_toward(self, hop, middle):
        low = self.me < self.n // 2
        for way in (0, 1):
            toward = low if way == 0 else jnp.logical_not(low)

            @pl.when(self.goes(hop, way) & (toward if middle else jnp.logical_not(toward)))
            def _(way=way):
                self.copy(self.slot(hop, way), hop, way).start()

    def take(self, hop, ways=(0, 1)):
        for way in ways:

            @pl.when(self.arrives(hop, way))
            def _(way=way):
                self.copy(self.slot(hop, way), hop, way).wait_recv()

    def relay(self, hop):
        for way in (0, 1):
            self.take(hop, (way,))
            if hop < self.n - 1:
                self.send(hop, (way,))

    def finish(self, first=0, last=None):
        for hop in range(first, self.n - 1 if last is None else last):
            for way in (0, 1):

                @pl.when(self.goes(hop, way))
                def _(way=way, hop=hop):
                    self.copy(self.slot(hop, way), hop, way).wait_send()


def own_then(own, buf):
    return lambda hop, slot: own if hop == 0 else buf.at[slot]


def line_sems(n):
    return [pltpu.SemaphoreType.DMA((2, n)), pltpu.SemaphoreType.DMA((n,))]


def vmem(count):
    return [pl.BlockSpec(memory_space=pltpu.VMEM)] * count


def params(collective_id=None):
    return pltpu.CompilerParams(
        collective_id=collective_id,
        has_side_effects=collective_id is not None,
        vmem_limit_bytes=VMEM_LIMIT,
    )


def plane(data_par):
    half = data_par // 2
    side = math.isqrt(half)
    return (side, half // side) if side * side == half else (1, half)


class PlaneGather:
    def __init__(self, n_data, buf, sems):
        self.ys, self.xs = plane(n_data)
        self.buf = buf
        self.s1a, self.s1b, self.r1a, self.r1b, self.s2a, self.s2b, self.r2a, self.r2b, self.cs, self.cr = sems
        me = lax.axis_index("dp")
        self.c = lax.rem(me, 2)
        self.x = lax.rem(me // 2, self.xs)
        self.y = me // (2 * self.xs)

    def move(self, src, dst, ssem, rsem, y, x, c):
        return pltpu.make_async_remote_copy(
            src_ref=src, dst_ref=dst, send_sem=ssem, recv_sem=rsem,
            device_id={"dp": (y * self.xs + x) * 2 + c}, device_id_type=MESH,
        )

    def east(self, o):
        return lax.rem(self.x + o + self.xs, self.xs)

    def north(self, o):
        return lax.rem(self.y + o + self.ys, self.ys)

    def first(self, k, back=False):
        out = []
        for o in range(1, self.xs):
            ref = self.buf.at[k, 0:2, self.y, self.east(-o) if back else self.x, self.c]
            out.append(self.move(ref, ref, self.s1a.at[k, o], self.r1a.at[k, o], self.y, self.east(o), self.c))
        for o in range(1, self.ys):
            ref = self.buf.at[k, 2:3, self.north(-o) if back else self.y, self.x, self.c]
            out.append(self.move(ref, ref, self.s1b.at[k, o], self.r1b.at[k, o], self.north(o), self.x, self.c))
        return out

    def second(self, k, back=False):
        out = []
        for o in range(1, self.ys):
            ref = self.buf.at[k, 0:2, self.north(-o) if back else self.y, :, self.c]
            out.append(self.move(ref, ref, self.s2a.at[k, o], self.r2a.at[k, o], self.north(o), self.x, self.c))
        for o in range(1, self.xs):
            ref = self.buf.at[k, 2:3, :, self.east(-o) if back else self.x, self.c]
            out.append(self.move(ref, ref, self.s2b.at[k, o], self.r2b.at[k, o], self.y, self.east(o), self.c))
        return out

    def third(self, k, back=False):
        ref = self.buf.at[k, :, :, :, 1 - self.c if back else self.c]
        return [self.move(ref, ref, self.cs.at[k], self.cr.at[k], self.y, self.x, 1 - self.c)]

    def stage(self, number, k):
        stages = (self.first, self.second, self.third)
        if number > 0:
            for copy in stages[number - 1](k, True):
                copy.wait_recv()
        if number < 3:
            for copy in stages[number](k):
                copy.start()

    def finish(self, k):
        for stage in (self.first, self.second, self.third):
            for copy in stage(k):
                copy.wait_send()

    @staticmethod
    def sems(n_data, count):
        ys, xs = plane(n_data)
        sem = pltpu.SemaphoreType.DMA
        xy = [sem((count, xs)), sem((count, ys))]
        return xy + xy + xy[::-1] + xy[::-1] + [sem((count,)), sem((count,))]


def near_hops(n):
    return min(2, n - 1)


def data_peers(n_data):
    mine = lax.axis_index("dp")
    return [{"dp": lax.rem(mine + off, n_data)} for off in range(1, n_data)]


def front_kernel(
    dims, n_data, x_ref, g_ref, win_ref, wo_ref, wd_ref, gain_ref, c_ref, st_ref,
    n1_out, q_out, k_out, v_out, lse_out, oc_out, wq_out, wt_out, g_near, n2_near, out_ref, dh_ref, n2_ref, dhb_ref, dgain_ref,
    n1_ref, q_ref, k_ref, v_ref, lse_ref, oc_ref, xbuf, wf, wpad, mask, opad, of_ref, h_ref, acc, dn2, zs, zr, ws, wr, gs, gr, ns, nr, as_, ar, os_, ko, *plane_sems,
):
    n, rows, heads, span = dims
    me = lax.axis_index("mp")
    cols = win_ref.shape[2]
    width = x_ref.shape[1]
    greet(line_peers(n, me) + data_peers(n_data))
    gather = LineGather(n, me, own_then(x_ref, xbuf), xbuf, zs, zr)
    whole = PlaneGather(n_data, wf, plane_sems)

    def place(k):
        return wf.at[k, :, whole.y, whole.x, whole.c]

    class Weights(LineGather):
        def copy(self, slot, hop, way):
            return pltpu.make_async_remote_copy(
                src_ref=place(slot), dst_ref=place(slot), send_sem=self.ssem.at[way, hop],
                recv_sem=self.rsem.at[slot], device_id={"mp": self.me + 1 - 2 * way}, device_id_type=MESH,
            )

    lines = Weights(n, me, None, None, ws, wr)
    gather_g = LineGather(n, me, own_then(g_ref, g_near), g_near, gs, gr)
    gather_n = LineGather(n, me, own_then(n2_ref, n2_near), n2_near, ns, nr)
    for k in range(3):
        place(n)[k] = win_ref[k].astype(BF16)
    place(me)[0] = wo_ref[...].astype(BF16)
    place(me)[1] = win_ref[3].astype(BF16)
    place(me)[2] = wd_ref[...].astype(BF16)
    lines.send(0)
    gather.send(0)
    whole.stage(0, n)
    sel = spread(cols, heads)
    xbuf[me] = x_ref[...]
    k_ref[...] = jnp.zeros_like(k_ref)
    v_ref[...] = jnp.zeros_like(v_ref)

    def matrix(k, m):
        value = wf[k, m]
        if value.shape[-2] % 16:
            return value.astype(F32).reshape(width, cols).astype(BF16)
        return value.reshape(width, cols)

    def arrivals(hop, do):
        def one(way, _):
            slot = me - hop + 2 * hop * way

            @pl.when((slot >= 0) & (slot < n))
            def _():
                do(slot)

            return 0

        lax.fori_loop(0, 2, one, 0)

    def forward(stage, hop):
        if 1 <= hop < n:
            arrivals(hop, lambda slot: whole.stage(stage, slot))

    whole.stage(1, n)
    whole.stage(0, me)
    whole.stage(2, n)
    whole.stage(3, n)
    lines.relay(1)
    gather.relay(1)
    forward(0, 1)
    whole.stage(1, me)
    for m in range(3):
        wpad[m] = nn(matrix(n, m), sel).astype(BF16)

    def keep_n1(slot):
        return pltpu.make_async_copy(n1_ref.at[slot], n1_out.at[slot], ko.at[slot])

    kept = [
        pltpu.make_async_copy(src, dst, ko.at[n + k])
        for k, (src, dst) in enumerate(
            ((q_ref, q_out), (k_ref, k_out), (v_ref, v_out), (lse_ref, lse_out), (oc_ref, oc_out))
        )
    ]

    def project(slot):
        x = xbuf[slot].astype(F32)
        scale = lax.rsqrt(jnp.mean(x * x, axis=-1, keepdims=True) + EPSILON)
        normed = (x * scale * gain_ref[0:1]).astype(BF16)
        n1_ref[slot] = normed
        keep_n1(slot).start()
        at = block_rows(slot, rows)
        for m, ref in enumerate((q_ref, k_ref, v_ref)):
            out = nn(normed, wpad[m])
            if m == 0:
                out = out * c_ref[...]
            out = out.astype(BF16)
            for h in range(heads):
                ref[h, at, :] = out[:, h * LANE : (h + 1) * LANE]

    project(me)

    def chunk(i):
        first = jnp.maximum(i - (span - 1), 0)
        at, keys = block_rows(i, rows), pl.ds(pl.multiple_of(first * rows, rows), span * rows)
        q_pos = i * rows + lax.broadcasted_iota(jnp.int32, mask.shape, 0)
        k_pos = first * rows + lax.broadcasted_iota(jnp.int32, mask.shape, 1)
        mask[...] = jnp.where((k_pos <= q_pos) & (k_pos >= st_ref[at, :]), 0.0, NEG)

        def head(h, _):
            scores = nt(q_ref[h, at, :], k_ref[h, keys, :]) + mask[...]
            top = jnp.max(scores, axis=-1, keepdims=True)
            raised = jnp.exp(scores - top)
            total = jnp.sum(raised, axis=-1, keepdims=True)
            prob = (raised * (1.0 / total)).astype(BF16)
            opad[h] = nn(prob, v_ref[h, keys, :]).astype(BF16)
            lse_ref[h, at, :] = top + jnp.log(total)
            return 0

        lax.fori_loop(0, heads, head, 0)
        wide = jnp.concatenate([opad[h] for h in range(heads)], axis=1)
        oc_ref[i] = nt(wide, sel).astype(BF16)

        @pl.when(i != me)
        def _():
            pltpu.make_async_remote_copy(
                src_ref=oc_ref.at[i], dst_ref=of_ref.at[me], send_sem=as_.at[i],
                recv_sem=ar.at[me], device_id={"mp": i}, device_id_type=MESH,
            ).start()

        @pl.when(i == me)
        def _():
            of_ref[me] = oc_ref[me]

    def ready(hop):
        def one(e, _):
            i = n - 1 - e
            low = jnp.maximum(i - (span - 1), 0)
            far = jnp.maximum(jnp.maximum(i - me, me - i), jnp.maximum(me - low, low - me))

            @pl.when((far <= 1) if hop == 1 else (far == hop))
            def _():
                chunk(i)

            return 0

        lax.fori_loop(0, n, one, 0)

    arrivals(1, project)
    ready(1)
    whole.stage(2, me)
    for hop in range(2, n):
        lines.relay(hop)
        forward(0, hop)
        forward(1, hop - 1)
        if hop == n - 1:
            forward(1, hop)
            forward(2, hop - 1)
        gather.relay(hop)
        if hop == 2:
            gather_g.send_toward(0, True)
        arrivals(hop, project)
        if hop == n - 1:
            for copy in kept[:3]:
                copy.start()
        ready(hop)
        if hop < n - 1:
            forward(2, hop - 1)
    gather_g.send_toward(0, False)
    forward(2, n - 1)
    for copy in kept[3:]:
        copy.start()

    def both(slot, _):
        whole.stage(3, slot)
        return 0

    lax.fori_loop(0, n, both, 0)
    keep_q = pltpu.make_async_copy(wf.at[n], wq_out, os_.at[0])
    keep_t = pltpu.make_async_copy(wf.at[me], wt_out, os_.at[1])
    keep_q.start()
    keep_t.start()
    h_ref[...] = x_ref[...].astype(F32) + nt(of_ref[me], matrix(me, 0))

    def outward(off, _):
        peer = lax.rem(me + off, n)
        copy = pltpu.make_async_remote_copy(
            src_ref=oc_ref.at[peer], dst_ref=of_ref.at[peer], send_sem=as_.at[peer],
            recv_sem=ar.at[peer], device_id={"mp": peer}, device_id_type=MESH,
        )
        copy.wait_recv()
        h_ref[...] += nt(of_ref[peer], matrix(peer, 0))
        copy.wait_send()
        return 0

    lax.fori_loop(1, n, outward, 0)
    h = h_ref[...]
    scale = lax.rsqrt(jnp.mean(h * h, axis=-1, keepdims=True) + EPSILON)
    n2_ref[...] = (h * scale * gain_ref[1:2]).astype(BF16)
    gather_n.send(0)
    acc[...] = h
    dn2[...] = jnp.zeros_like(dn2)

    def hidden(j, _):
        up, down = matrix(j, 1), matrix(j, 2)
        gate = nn(n2_ref[...], up)
        sig = 1.0 / (1.0 + jnp.exp(-gate))
        acc[...] += nt((gate * sig).astype(BF16), down)
        dz = nn(g_ref[...], down)
        da = (dz * (sig * (1.0 + gate * (1.0 - sig)))).astype(BF16)
        dn2[...] += nt(da, up)
        return 0

    lax.fori_loop(0, n, hidden, 0)
    out_ref[...] = acc[...].astype(BF16)
    h = h_ref[...]
    scale = lax.rsqrt(jnp.mean(h * h, axis=-1, keepdims=True) + EPSILON)
    unit = h * scale
    grad = dn2[...]
    dgain_ref[...] = jnp.sum(grad * unit, axis=0, keepdims=True)
    du = grad * gain_ref[1:2]
    dh = g_ref[...].astype(F32) + scale * (du - unit * jnp.mean(du * unit, axis=-1, keepdims=True))
    dh_ref[...] = dh
    dhb_ref[...] = dh.astype(BF16)
    gather_g.take(1)
    gather_n.take(1)
    gather_g.finish(0, 1)
    gather_n.finish(0, 1)
    gather.finish()
    lines.finish()

    def sent(k, _):
        whole.finish(k)
        return 0

    lax.fori_loop(0, n + 1, sent, 0)
    keep_q.wait()
    keep_t.wait()
    for copy in kept:
        copy.wait()
    for slot in range(n):
        keep_n1(slot).wait()


def front(dims, x, g, w_in, w_out, w_down, gains, c_row, starts):
    n, rows, heads, span = dims
    n_data = lax.axis_size("dp")
    own_rows, cols = w_in.shape[1:]
    width = x.shape[1]
    count = n * rows
    ys, xs = plane(n_data)
    head_out = jax.ShapeDtypeStruct((heads, count, LANE), BF16)
    kept = jax.ShapeDtypeStruct((3, ys, xs, 2, own_rows, cols), BF16)
    own = jax.ShapeDtypeStruct((rows, width), BF16)
    sem = pltpu.SemaphoreType.DMA
    return pl.pallas_call(
        functools.partial(front_kernel, dims, n_data),
        out_shape=(
            jax.ShapeDtypeStruct((n, rows, width), BF16),
            head_out, head_out, head_out,
            jax.ShapeDtypeStruct((heads, count, 1), F32),
            jax.ShapeDtypeStruct((n, rows, cols), BF16),
            kept, kept,
            jax.ShapeDtypeStruct((n, rows, width), BF16),
            jax.ShapeDtypeStruct((n, rows, width), BF16),
            own,
            jax.ShapeDtypeStruct((rows, width), F32),
            own, own,
            jax.ShapeDtypeStruct((1, width), F32),
        ),
        in_specs=vmem(8),
        out_specs=[pl.BlockSpec(memory_space=pl.ANY)] * 10 + vmem(5),
        scratch_shapes=[
            pltpu.VMEM((n, rows, width), BF16),
            *[pltpu.VMEM((heads, count, LANE), BF16)] * 3,
            pltpu.VMEM((heads, count, 1), F32),
            pltpu.VMEM((n, rows, cols), BF16),
            pltpu.VMEM((n, rows, width), BF16),
            pltpu.VMEM((n + 1, *kept.shape), BF16),
            pltpu.VMEM((3, width, heads * LANE), BF16),
            pltpu.VMEM((rows, span * rows), F32),
            pltpu.VMEM((heads, rows, LANE), BF16),
            pltpu.VMEM((n, rows, cols), BF16),
            pltpu.VMEM((rows, width), F32), pltpu.VMEM((rows, width), F32), pltpu.VMEM((rows, width), F32),
            *line_sems(n), *line_sems(n), *line_sems(n), *line_sems(n),
            sem((n,)), sem((n,)), sem((2,)), sem((n + 5,)),
            *PlaneGather.sems(n_data, n + 1),
        ],
        compiler_params=params(1),
        name="front",
    )(x, g, w_in, w_out, w_down, gains, c_row, starts)


def back_kernel(
    dims, own_ref, c_ref, st_ref, q_hbm, k_hbm, v_hbm, lse_hbm, w_hbm, g_near,
    dx_ref, dc_ref, dhb_out, g_mid,
    q_ref, k_ref, v_ref, lse_ref, dhb_ref, w_ref, wpad, mask, do_ref, dq_ref, dk_ref, dv_ref, zs, zr, gs, gr, w_sem, ko,
):
    n, rows, heads, span = dims
    me = lax.axis_index("mp")
    takes = [
        pltpu.make_async_copy(src, dst, w_sem.at[k])
        for k, (src, dst) in enumerate(
            ((w_hbm.at[0], w_ref), (q_hbm, q_ref), (k_hbm, k_ref), (v_hbm, v_ref), (lse_hbm, lse_ref))
        )
    ]
    for copy in takes:
        copy.start()
    greet(line_peers(n, me))
    gather = LineGather(n, me, own_then(own_ref, dhb_ref), dhb_ref, zs, zr)
    gather.send(0)
    gather_g = LineGather(n, me, lambda hop, slot: g_near.at[slot], g_mid, gs, gr)
    dhb_ref[me] = own_ref[...]
    sel = spread(w_ref.shape[1], heads)
    for copy in takes:
        copy.wait()
    wpad[...] = nn(w_ref[...], sel).astype(BF16)
    dk_ref[...] = jnp.zeros_like(dk_ref)
    dv_ref[...] = jnp.zeros_like(dv_ref)
    dc_ref[...] = jnp.zeros_like(dc_ref)

    def squeeze(ref, at):
        wide = jnp.concatenate([ref[h, at, :].astype(BF16) for h in range(heads)], axis=1)
        return nt(wide, sel).astype(BF16)

    def keep(i):
        return pltpu.make_async_copy(dhb_ref.at[i], dhb_out.at[i], ko.at[i])

    def chunk(i):
        keep(i).start()
        first = jnp.maximum(i - (span - 1), 0)
        at, keys = block_rows(i, rows), pl.ds(pl.multiple_of(first * rows, rows), span * rows)
        q_pos = i * rows + lax.broadcasted_iota(jnp.int32, mask.shape, 0)
        k_pos = first * rows + lax.broadcasted_iota(jnp.int32, mask.shape, 1)
        mask[...] = jnp.where((k_pos <= q_pos) & (k_pos >= st_ref[at, :]), 0.0, NEG)
        grad = nn(dhb_ref[i], wpad[...]).astype(BF16)
        for h in range(heads):
            do_ref[h] = grad[:, h * LANE : (h + 1) * LANE]

        def head(h, _):
            query = q_ref[h, at, :]
            scores = nt(query, k_ref[h, keys, :]) + mask[...]
            prob = jnp.exp(scores - lse_ref[h, at, :])
            dp = nt(do_ref[h], v_ref[h, keys, :])
            inner = jnp.sum(prob * dp, axis=-1, keepdims=True)
            ds = (prob * (dp - inner)).astype(BF16)
            dq = nn(ds, k_ref[h, keys, :])
            dk_ref[h, keys, :] += tn(ds, query)
            dv_ref[h, keys, :] += tn(prob.astype(BF16), do_ref[h])
            dc_ref[...] += jnp.sum(dq * query.astype(F32), axis=0, keepdims=True)
            dq_ref[h] = (dq * c_ref[:, :LANE]).astype(BF16)
            return 0

        lax.fori_loop(0, heads, head, 0)
        dx_ref[0, i] = squeeze(dq_ref, slice(None))

    def event(e, _):
        hop, way = (e + 1) // 2, lax.rem(e + 1, 2)
        i = me - hop + 2 * hop * way

        @pl.when((way == 0) & (hop > 0))
        def _():
            for fixed in range(1, n):

                @pl.when(hop == fixed)
                def _(fixed=fixed):
                    gather.relay(fixed)

        @pl.when((i >= 0) & (i < n))
        def _():
            chunk(i)

        return 0

    lax.fori_loop(0, 2 * n - 1, event, 0)
    if n > 2:
        gather_g.send(1)

    def close(i, _):
        at = block_rows(i, rows)
        dx_ref[1, i] = squeeze(dk_ref, at)
        dx_ref[2, i] = squeeze(dv_ref, at)
        return 0

    lax.fori_loop(0, n, close, 0)
    gather.finish()
    if n > 2:
        gather_g.take(2)
        gather_g.finish(1, 2)
    for i in range(n):
        keep(i).wait()


def back(dims, q, k, v, lse, dhb, c_row, starts, w_tail, g_near):
    n, rows, heads, span = dims
    width, cols = w_tail.shape[1:]
    every = jax.ShapeDtypeStruct((n, rows, width), BF16)
    sem = pltpu.SemaphoreType.DMA
    anywhere = pl.BlockSpec(memory_space=pl.ANY)
    return pl.pallas_call(
        functools.partial(back_kernel, dims),
        out_shape=(
            jax.ShapeDtypeStruct((3, n, rows, cols), BF16),
            jax.ShapeDtypeStruct((1, LANE), F32),
            every, every,
        ),
        in_specs=vmem(3) + [anywhere] * 6,
        out_specs=vmem(2) + [anywhere] * 2,
        scratch_shapes=[
            *[pltpu.VMEM((heads, n * rows, LANE), BF16)] * 3,
            pltpu.VMEM((heads, n * rows, 1), F32),
            pltpu.VMEM((n, rows, width), BF16),
            pltpu.VMEM((width, cols), BF16),
            pltpu.VMEM((width, heads * LANE), BF16),
            pltpu.VMEM((rows, span * rows), F32),
            pltpu.VMEM((heads, rows, LANE), BF16),
            pltpu.VMEM((heads, rows, LANE), BF16),
            pltpu.VMEM((heads, n * rows, LANE), F32),
            pltpu.VMEM((heads, n * rows, LANE), F32),
            *line_sems(n), *line_sems(n),
            sem((5,)), sem((n,)),
        ],
        compiler_params=params(2),
        name="back",
    )(dhb, c_row, starts, q, k, v, lse, w_tail, g_near)


def halves(value):
    high = value.astype(BF16)
    return high, (value - high.astype(F32)).astype(BF16)


def dot_split(small, big, contract):
    count = small.shape[0]
    high, low = halves(small)
    big_high, big_low = halves(big)
    both = contract(jnp.concatenate([high.astype(F32), low.astype(F32)], axis=0).astype(BF16), big_high)
    return both[:count] + both[count:] + contract(high, big_low)


class PlaneScatter:
    def __init__(self, n_data, gb, core, a1, b1, a2, b2, sems):
        self.ys, self.xs = plane(n_data)
        self.gb, self.core, self.a1, self.b1, self.a2, self.b2 = gb, core, a1, b1, a2, b2
        (self.c_s, self.c_r, self.s1, self.ra1, self.rb1, self.s2, self.ra2, self.rb2) = sems
        me = lax.axis_index("dp")
        self.c = lax.rem(me, 2)
        self.x = lax.rem(me // 2, self.xs)
        self.y = me // (2 * self.xs)
        self.half = gb.shape[0] // 2

    def send(self, src, dst, ssem, rsem, y, x, c):
        return pltpu.make_async_remote_copy(
            src_ref=src, dst_ref=dst, send_sem=ssem, recv_sem=rsem,
            device_id={"dp": (y * self.xs + x) * 2 + c}, device_id_type=MESH,
        )

    def copies_core(self):
        other = 1 - self.c
        src = self.gb.at[:, :, :, other]
        return [self.send(src, self.core, self.c_s, self.c_r, self.y, self.x, other)]

    def copies_one(self):
        out, h = [], self.half
        for o in range(1, self.xs):
            to = lax.rem(self.x + o, self.xs)
            src = self.core.at[:h, :, to]
            out.append(self.send(src, self.a1.at[o - 1], self.s1.at[0, o], self.ra1.at[o], self.y, to, self.c))
        for o in range(1, self.ys):
            to = lax.rem(self.y + o, self.ys)
            src = self.core.at[h:, to]
            out.append(self.send(src, self.b1.at[o - 1], self.s1.at[1, o], self.rb1.at[o], to, self.x, self.c))
        return out

    def copies_two(self):
        out, h = [], self.half
        for o in range(1, self.ys):
            to = lax.rem(self.y + o, self.ys)
            src = self.core.at[:h, to, self.x]
            out.append(self.send(src, self.a2.at[o - 1], self.s2.at[0, o], self.ra2.at[o], to, self.x, self.c))
        for o in range(1, self.xs):
            to = lax.rem(self.x + o, self.xs)
            src = self.core.at[h:, self.y, to]
            out.append(self.send(src, self.b2.at[o - 1], self.s2.at[1, o], self.rb2.at[o], self.y, to, self.c))
        return out

    def start(self, copies):
        for copy in copies:
            copy.start()

    def arrive(self, copies):
        for copy in copies:
            copy.wait_recv()

    def sum_core(self):
        self.arrive(self.copies_core())

        def one(i, _):
            m, rest = i // (self.ys * self.xs), lax.rem(i, self.ys * self.xs)
            y, x = rest // self.xs, lax.rem(rest, self.xs)
            total = self.core[m, y, x].astype(F32) + self.gb[m, y, x, self.c].astype(F32)
            self.core[m, y, x] = total.astype(BF16)
            return 0

        lax.fori_loop(0, self.gb.shape[0] * self.ys * self.xs, one, 0)

    def sum_one(self):
        self.arrive(self.copies_one())
        h = self.half

        def along_y(i, _):
            m, y = i // self.ys, lax.rem(i, self.ys)
            total = self.core[m, y, self.x].astype(F32)
            for o in range(1, self.xs):
                total += self.a1[o - 1, m, y].astype(F32)
            self.core[m, y, self.x] = total.astype(BF16)
            return 0

        def along_x(i, _):
            m, x = i // self.xs, lax.rem(i, self.xs)
            total = self.core[h + m, self.y, x].astype(F32)
            for o in range(1, self.ys):
                total += self.b1[o - 1, m, x].astype(F32)
            self.core[h + m, self.y, x] = total.astype(BF16)
            return 0

        lax.fori_loop(0, h * self.ys, along_y, 0)
        lax.fori_loop(0, h * self.xs, along_x, 0)

    def sum_two(self, put):
        self.arrive(self.copies_two())
        for m in range(self.half):
            total = self.core[m, self.y, self.x].astype(F32)
            for o in range(1, self.ys):
                total += self.a2[o - 1, m].astype(F32)
            put(m, total)
            total = self.core[self.half + m, self.y, self.x].astype(F32)
            for o in range(1, self.xs):
                total += self.b2[o - 1, m].astype(F32)
            put(self.half + m, total)

    def finish(self):
        for copy in self.copies_core() + self.copies_one() + self.copies_two():
            copy.wait_send()

    @staticmethod
    def scratch(n_data, count, rows, cols):
        ys, xs = plane(n_data)
        h = count // 2
        sem = pltpu.SemaphoreType.DMA
        return [
            pltpu.VMEM((count, ys, xs, 2, rows, cols), BF16),
            pltpu.VMEM((count, ys, xs, rows, cols), BF16),
            pltpu.VMEM((max(xs - 1, 1), h, ys, rows, cols), BF16),
            pltpu.VMEM((max(ys - 1, 1), h, xs, rows, cols), BF16),
            pltpu.VMEM((max(ys - 1, 1), h, rows, cols), BF16),
            pltpu.VMEM((max(xs - 1, 1), h, rows, cols), BF16),
            sem, sem, sem((2, max(xs, ys))), sem((xs,)), sem((ys,)),
            sem((2, max(xs, ys))), sem((ys,)), sem((xs,)),
        ]


class Exchange:
    def __init__(self, axis, size, src_of, dst, ssem, rsem):
        self.axis, self.size, self.src_of, self.dst, self.ssem, self.rsem = axis, size, src_of, dst, ssem, rsem
        self.me = lax.axis_index(axis)

    def copy(self, peer, slot):
        return pltpu.make_async_remote_copy(
            src_ref=self.src_of(peer), dst_ref=self.dst.at[slot], send_sem=self.ssem.at[peer],
            recv_sem=self.rsem.at[slot], device_id={self.axis: peer}, device_id_type=MESH,
        )

    def each(self, do):
        def one(off, _):
            do(lax.rem(self.me + off, self.size))
            return 0

        lax.fori_loop(1, self.size, one, 0)

    def start(self):
        self.each(lambda peer: self.copy(peer, self.me).start())

    def arrive(self):
        self.each(lambda peer: self.copy(peer, peer).wait_recv())

    def finish(self):
        self.each(lambda peer: self.copy(peer, peer).wait_send())


def total_of(ref, size):
    def one(i, total):
        return total + ref[i]

    return lax.fori_loop(1, size, one, ref[0])


FIRST, SECOND = (0, 1, 2, 4), (3, 5)


class Factors:
    def __init__(self, n, n_data, group, index, ft, m_ref, basis, right, refs):
        self.group, self.index, self.ft, self.m, self.basis, self.right = group, index, ft, m_ref, basis, right
        self.send, self.got, self.line, self.full, self.rgot = refs[:5]
        l_s, l_r, z_s, z_r, a_s, a_r, r_s, r_r = refs[5:]
        self.n, self.n_data = n, n_data
        self.tiles = basis.shape[2] // LANE
        self.per = self.send.shape[1]
        self.mine, self.me = lax.axis_index("dp"), lax.axis_index("mp")
        mine, me = self.mine, self.me
        self.ex_left = Exchange("dp", n_data, lambda peer: self.send.at[peer], self.got, l_s, l_r)
        self.ex_line = Exchange("mp", n, lambda peer: self.line.at[me], self.line, z_s, z_r)
        self.ex_all = Exchange("dp", n_data, lambda peer: self.full.at[mine], self.full, a_s, a_r)
        self.ex_right = Exchange("dp", n_data, lambda peer: self.rgot.at[mine], self.rgot, r_s, r_r)

    def start(self):
        size = len(self.group) * self.tiles
        for tile in range(size, self.n_data * self.per):
            self.send[tile // self.per, tile % self.per] = jnp.zeros((8, LANE), F32)

        def rows_of(k, _):
            m = self.index(k)
            rows_left = dot_split(self.ft[m], self.m[m], nn)
            for t in range(self.tiles):
                tile = k * self.tiles + t
                self.send[tile // self.per, lax.rem(tile, self.per)] = rows_left[:, t * LANE : (t + 1) * LANE]
            return 0

        lax.fori_loop(0, len(self.group), rows_of, 0)
        self.got[self.mine] = self.send[self.mine]
        self.ex_left.start()

    def along_line(self):
        self.ex_left.arrive()
        self.line[self.me] = total_of(self.got, self.n_data)
        self.ex_line.start()

    def spread_out(self):
        self.ex_line.arrive()
        self.full[self.mine] = total_of(self.line, self.n)
        self.ex_all.start()

    def orthonormal(self):
        self.ex_all.arrive()
        tiles, per = self.tiles, self.per
        basis = jnp.stack(
            [
                jnp.concatenate([self.full[t // per, t % per] for t in range(k * tiles, (k + 1) * tiles)], axis=1)
                for k in range(len(self.group))
            ]
        )
        row = lax.broadcasted_iota(jnp.int32, (1, 8, 1), 1)
        for index in range(8):
            vector = basis[:, index : index + 1, :]
            vector = vector * lax.rsqrt(jnp.sum(vector * vector, axis=-1, keepdims=True) + 1e-12)
            onto = jnp.where(row > index, jnp.sum(basis * vector, axis=-1, keepdims=True), 0.0)
            basis = jnp.where(row == index, vector, basis - onto * vector)
        for k, m in enumerate(self.group):
            self.basis[m] = basis[k]

        def rows_of(k, _):
            m = self.index(k)
            self.rgot[self.mine, k] = dot_split(self.basis[m], self.m[m], nt)
            return 0

        lax.fori_loop(0, len(self.group), rows_of, 0)
        self.ex_right.start()

    def close(self):
        self.ex_right.arrive()
        total = total_of(self.rgot, self.n_data)
        for k, m in enumerate(self.group):
            self.right[m] = total[k]

    def finish(self):
        for exchange in (self.ex_left, self.ex_line, self.ex_all, self.ex_right):
            exchange.finish()

    @staticmethod
    def scratch(n, n_data, count, width, cols):
        sem = pltpu.SemaphoreType.DMA
        per = -(-(count * width // LANE) // n_data)
        tiles = (per, 8, LANE)
        return [
            pltpu.VMEM((n_data, *tiles), F32), pltpu.VMEM((n_data, *tiles), F32),
            pltpu.VMEM((n, *tiles), F32), pltpu.VMEM((n_data, *tiles), F32),
            pltpu.VMEM((n_data, count, 8, cols), F32),
            sem((n_data,)), sem((n_data,)), sem((n,)), sem((n,)),
            sem((n_data,)), sem((n_data,)), sem((n_data,)), sem((n_data,)),
        ]


def grads_kernel(
    dims, n_data, scaling, n1_ref, n2_ref, n2_near, dhb_ref, g_ref, g_near, g_mid, dx_hbm, oc_hbm, wqkv_hbm, wtail_hbm,
    err_ref, x_ref, dh_ref, gain_ref, dgain2_ref, dscale_ref, ft_ref,
    gin_sum, gout_sum, gin_ref, basis_ref, right_ref, small_ref, m_out, n2_far, g_far,
    abuf, dx_ref, wbuf, sbuf, lbuf, m_ref, srecv, szrecv,
    fs, ns_, nr_, gs_, gr_, gts, gtr, nts, ntr, ss, ls, es, ms, g_s, g_r, gz_s, gz_r, *refs,
):
    n, rows, heads, span = dims
    hops_g = near_hops(n)
    me, mine = lax.axis_index("mp"), lax.axis_index("dp")
    width, cols = wbuf.shape[1:]
    tiles = width // LANE
    sizes = (14, 14, 13, 13)
    cuts = [sum(sizes[:k]) for k in range(5)]
    parts = [refs[cuts[k] : cuts[k + 1]] for k in range(4)]

    def load(m):
        return pltpu.make_async_copy(err_ref.at[m], m_ref.at[m], es.at[m])

    def save(m):
        return pltpu.make_async_copy(m_ref.at[m], m_out.at[m], ms.at[m])

    take_dx = pltpu.make_async_copy(dx_hbm, dx_ref, fs.at[0])
    take_oc = pltpu.make_async_copy(oc_hbm, dx_ref.at[2], fs.at[1])
    take_qkv = pltpu.make_async_copy(wqkv_hbm, wbuf, fs.at[2])
    take_tail = pltpu.make_async_copy(wtail_hbm, wbuf, fs.at[3])
    take_dhb = pltpu.make_async_copy(dhb_ref, abuf.at[0], fs.at[4])
    take_n1 = pltpu.make_async_copy(n1_ref, abuf.at[1], fs.at[5])
    take_dx.start()
    take_qkv.start()
    take_n1.start()
    for m in range(6):
        load(m).start()
    take_dhb.start()
    greet(line_peers(n, me) + data_peers(n_data))
    scatter_1 = PlaneScatter(n_data, *parts[0][:6], parts[0][6:])
    scatter_2 = PlaneScatter(n_data, *parts[1][:6], parts[1][6:])
    chain_1 = Factors(n, n_data, FIRST, lambda k: k + k // 3, ft_ref, m_ref, basis_ref, right_ref, parts[2])
    chain_2 = Factors(n, n_data, SECOND, lambda k: 3 + 2 * k, ft_ref, m_ref, basis_ref, right_ref, parts[3])
    gb_1, gb_2 = parts[0][0], parts[1][0]
    ex_small = Exchange("dp", n_data, lambda peer: srecv.at[mine], srecv, g_s, g_r)
    ex_small_line = Exchange("mp", n, lambda peer: szrecv.at[me], szrecv, gz_s, gz_r)

    def follow(near, far, hops):
        return lambda hop, slot: near.at[slot] if hop <= hops else far.at[slot]

    gather_n = LineGather(n, me, follow(n2_near, n2_far, 1), n2_far, nts, ntr)
    gather_g = LineGather(n, me, follow(g_mid, g_far, hops_g), g_far, gts, gtr)

    def bring(step, which):
        gather, hops = ((gather_n, 1), (gather_g, hops_g))[which]
        hop = hops + step
        if step == 0 and hop < n - 1:
            gather.send(hop)
        elif step > 0 and hop < n - 1:
            gather.relay(hop)

    bring(0, 0)

    def away(i):
        return jnp.maximum(i - me, me - i)

    def take_inputs(far, do):
        for i in range(n):
            d = away(i)
            if far:
                cases = ((0, n2_far, d > 1), (1, g_mid, d == 2), (1, g_far, d > 2))
            else:
                cases = ((0, n2_near, d == 1), (1, g_near, d == 1))
            for k, src, hit in cases:

                @pl.when(hit)
                def _(k=k, src=src, i=i):
                    do(pltpu.make_async_copy(src.at[i], abuf.at[k, i], (ns_, gs_)[k].at[i]))

        if not far:
            do(pltpu.make_async_copy(n2_ref, abuf.at[0, me], ns_.at[me]))
            do(pltpu.make_async_copy(g_ref, abuf.at[1, me], gs_.at[me]))


    def own(e, _):
        i = jnp.where(lax.rem(e, 2) == 0, n - 1 - e // 2, e // 2)
        total = nt(dx_ref[0, i], wbuf[0])
        total += nt(dx_ref[1, i], wbuf[1])
        total += nt(dx_ref[2, i], wbuf[2])

        @pl.when(i == me)
        def _():
            gin_ref[...] = total

        @pl.when(i != me)
        def _():
            sbuf[i] = total.astype(BF16)

        return 0

    take_dx.wait()
    take_qkv.wait()
    lax.fori_loop(0, n, own, 0)
    take_tail.start()

    def copy(i, way, here=False):
        slot = i if way == 0 else jnp.where(i == (me if here else me - 1), n, i)
        return pltpu.make_async_remote_copy(
            src_ref=sbuf.at[i], dst_ref=lbuf.at[slot], send_sem=ss.at[i], recv_sem=ls.at[slot],
            device_id={"mp": me + 1 - 2 * way}, device_id_type=MESH,
        )

    def launch():
        @pl.when(me == 0)
        def _():
            for i in range(n - 1, 0, -1):
                copy(i, 0).start()

        @pl.when(me == n - 1)
        def _():
            for i in range(n - 1):
                copy(i, 1).start()

    def relay(r):
        for way in (0, 1):
            place = me if way == 0 else n - 1 - me
            i = n - 1 - r + me if way == 0 else r - (n - 1 - me)

            @pl.when((place >= 1) & (place <= r))
            def _(i=i, way=way):
                copy(i, way, True).wait_recv()
                sbuf[i] = (sbuf[i].astype(F32) + lbuf[i].astype(F32)).astype(BF16)
                copy(i, way).start()

    launch()
    bring(0, 1)

    def hidden(i):
        gate = nn(abuf[0, i], wbuf[1])
        sig = 1.0 / (1.0 + jnp.exp(-gate))
        dx_ref[0, i] = (gate * sig).astype(BF16)
        dz = nn(abuf[1, i], wbuf[2])
        dx_ref[1, i] = (dz * (sig * (1.0 + gate * (1.0 - sig)))).astype(BF16)

    def hiddens(far):
        def one(i, _):
            @pl.when((away(i) > 1) if far else (away(i) <= 1))
            def _():
                hidden(i)

            return 0

        lax.fori_loop(0, n, one, 0)

    def flat(value):
        return value.reshape(n * rows, value.shape[-1])

    def weight(m, gb, k, a, b):
        left, right = flat(a), flat(b)
        load(m).wait()
        m_ref[m] = scaling * tn(right, left) + m_ref[m]
        gb[k] = tn(left, right).reshape(gb.shape[1:]).astype(BF16)

    def inputs(m, _):
        weight(m, gb_1, m, abuf[1], dx_ref[m])
        return 0

    take_n1.wait()
    lax.fori_loop(0, 3, inputs, 0)
    take_oc.start()
    take_dhb.wait()
    take_oc.wait()
    weight(4, gb_1, 3, abuf[0], dx_ref[2])
    chain_1.start()
    scatter_1.start(scatter_1.copies_core())
    take_inputs(False, lambda c: c.start())
    bring(1, 0)
    bring(1, 1)
    relay(1)
    chain_1.along_line()
    scatter_1.sum_core()
    scatter_1.start(scatter_1.copies_one())
    take_tail.wait()
    take_inputs(False, lambda c: c.wait())
    hiddens(False)
    for r in range(2, n - 1):
        relay(r)
        bring(r, 0)
        bring(r, 1)
    gather_n.take(n - 1)
    gather_g.take(n - 1)
    take_inputs(True, lambda c: c.start())
    scatter_1.sum_one()
    scatter_1.start(scatter_1.copies_two())
    take_inputs(True, lambda c: c.wait())
    hiddens(True)

    def late(k, _):
        weight(3 + 2 * k, gb_2, k, abuf[k], dx_ref[1 - k])
        return 0

    lax.fori_loop(0, 2, late, 0)
    chain_2.start()
    scatter_2.start(scatter_2.copies_core())
    for m in range(6):
        save(m).start()
    chain_1.spread_out()


    @pl.when(me > 0)
    def _():
        copy(me, 0).wait_recv()
        gin_ref[...] += lbuf[me].astype(F32)

    @pl.when(me < n - 1)
    def _():
        copy(me, 1, True).wait_recv()
        gin_ref[...] += lbuf[n].astype(F32)

    chain_2.along_line()
    x = x_ref[...].astype(F32)
    scale = lax.rsqrt(jnp.mean(x * x, axis=-1, keepdims=True) + EPSILON)
    unit = x * scale
    grad = gin_ref[...]
    dgain = jnp.sum(grad * unit, axis=0, keepdims=True)
    srecv[mine] = jnp.zeros(srecv.shape[1:], F32)
    for t in range(tiles):
        at = slice(t * LANE, (t + 1) * LANE)
        srecv[mine, t // 8, t % 8 : t % 8 + 1, :] = scaling * dgain[:, at]
        t2 = tiles + t
        srecv[mine, t2 // 8, t2 % 8 : t2 % 8 + 1, :] = scaling * dgain2_ref[:, at]
    t3 = 2 * tiles
    srecv[mine, t3 // 8, t3 % 8 : t3 % 8 + 1, :] = scaling * dscale_ref[...]
    ex_small.start()
    scatter_2.sum_core()
    scatter_2.start(scatter_2.copies_one())
    chain_2.spread_out()
    du = grad * gain_ref[0:1]
    gin_ref[...] = dh_ref[...] + scale * (du - unit * jnp.mean(du * unit, axis=-1, keepdims=True))
    chain_1.orthonormal()
    ex_small.arrive()
    szrecv[me] = total_of(srecv, n_data)
    ex_small_line.start()
    chain_2.orthonormal()

    def put_1(k, value):
        if k < 3:
            gin_sum[k] = scaling * value
        else:
            gout_sum[0] = scaling * value

    def put_2(k, value):
        (gout_sum if k else gin_sum)[1 if k else 3] = scaling * value

    scatter_1.sum_two(put_1)
    chain_1.close()
    scatter_2.sum_one()
    scatter_2.start(scatter_2.copies_two())
    ex_small_line.arrive()
    small_ref[...] = total_of(szrecv, n)
    chain_2.close()
    scatter_2.sum_two(put_2)

    for i in range(n):

        @pl.when(me < i)
        def _(i=i):
            copy(i, 0).wait_send()

        @pl.when(me > i)
        def _(i=i):
            copy(i, 1).wait_send()

    chain_1.finish()
    chain_2.finish()
    ex_small.finish()
    ex_small_line.finish()
    scatter_1.finish()
    scatter_2.finish()
    gather_g.finish(hops_g)
    gather_n.finish(1)
    for m in range(6):
        save(m).wait()


def grads(dims, scaling, hbm, x, dh, gain, dgain2, dscale, ft):
    n, rows = dims[:2]
    n_data = lax.axis_size("dp")
    width, cols = hbm[-2].shape[1:]
    own_rows = width // n_data
    sem = pltpu.SemaphoreType.DMA
    small = -(-(2 * width // LANE + 1) // 8)
    far = jax.ShapeDtypeStruct((n, rows, width), BF16)

    def f32(*shape):
        return pltpu.VMEM(shape, F32)

    def out(*shape):
        return jax.ShapeDtypeStruct(shape, F32)

    return pl.pallas_call(
        functools.partial(grads_kernel, dims, n_data, scaling),
        out_shape=(
            out(4, own_rows, cols), out(2, own_rows, cols), out(rows, width),
            out(6, 8, width), out(6, 8, cols), out(small, 8, LANE),
            out(6, cols, width), far, far,
        ),
        in_specs=[pl.BlockSpec(memory_space=pl.ANY)] * len(hbm) + vmem(6),
        out_specs=vmem(6) + [pl.BlockSpec(memory_space=pl.ANY)] * 3,
        scratch_shapes=[
            pltpu.VMEM((2, n, rows, width), BF16),
            pltpu.VMEM((3, n, rows, cols), BF16),
            pltpu.VMEM((3, width, cols), BF16),
            pltpu.VMEM((n, rows, width), BF16),
            pltpu.VMEM((n + 1, rows, width), BF16),
            f32(6, cols, width),
            f32(n_data, small, 8, LANE), f32(n, small, 8, LANE),
            sem((6,)), sem((n,)), sem((n,)), sem((n,)), sem((n,)),
            *line_sems(n), *line_sems(n), sem((n,)), sem((n + 1,)), sem((6,)), sem((6,)),
            sem((n_data,)), sem((n_data,)), sem((n,)), sem((n,)),
            *PlaneScatter.scratch(n_data, 4, own_rows, cols),
            *PlaneScatter.scratch(n_data, 2, own_rows, cols),
            *Factors.scratch(n, n_data, 4, width, cols),
            *Factors.scratch(n, n_data, 2, width, cols),
        ],
        compiler_params=params(3),
        name="grads",
    )(*hbm, x, dh, gain, dgain2, dscale, ft)[:7]


def outer(a, b):
    (ah, al), (bh, bl) = halves(a), halves(b)
    left = jnp.concatenate([ah.astype(F32), al.astype(F32), ah.astype(F32)], axis=0).astype(BF16)
    right = jnp.concatenate([bh.astype(F32), bh.astype(F32), bl.astype(F32)], axis=0).astype(BF16)
    return tn(left, right)


def close_kernel(
    m_ref, right_ref, basis_ref, mine_ref, mom_in_ref, w_in_ref, mom_out_ref, w_out_ref, w_down_ref,
    gin_ref, out_ref, gw_ref, gw2_ref,
    err_ref, new_in_ref, mom_in_new_ref, new_out_ref, mom_out_new_ref, gin_out, out_out, gw_out, gw2_out,
):
    k = pl.program_id(0)
    right, mine = right_ref[0], mine_ref[0]
    err_ref[0] = m_ref[0] - outer(right, basis_ref[0])
    gin_out[...] = gin_ref[...]
    out_out[...] = out_ref[...]
    gw_out[...] = gw_ref[...]
    gw2_out[...] = gw2_ref[...]
    step = outer(mine, right)

    @pl.when(k < 4)
    def _():
        moment = MOMENTUM * mom_in_ref[0] + step
        mom_in_new_ref[0] = moment
        new_in_ref[0] = w_in_ref[0] - RATE * moment

    for index, ref in ((4, w_out_ref), (5, w_down_ref)):

        @pl.when(k == index)
        def _(ref=ref):
            moment = MOMENTUM * mom_out_ref[0] + step
            mom_out_new_ref[0] = moment
            new_out_ref[0] = ref[...] - RATE * moment


def close(m, right, basis, mine, mom_in, w_in, mom_out, w_out, w_down, grad_input, output, grad_in, grad_out):
    cols, width = m.shape[1:]
    own_rows = w_in.shape[1]
    quarter = grad_input.shape[0] // 4

    def spec(*shape):
        return pl.BlockSpec((1, *shape), lambda i: (i, 0, 0))

    into = pl.BlockSpec((1, own_rows, cols), lambda i: (jnp.minimum(i, 3), 0, 0))
    out = pl.BlockSpec((1, own_rows, cols), lambda i: (jnp.maximum(i - 4, 0), 0, 0))
    whole = pl.BlockSpec((own_rows, cols), lambda i: (0, 0))
    part = pl.BlockSpec((quarter, width), lambda i: (jnp.minimum(i, 3), 0))

    def like(x):
        return jax.ShapeDtypeStruct(x.shape, x.dtype)

    return pl.pallas_call(
        close_kernel,
        grid=(6,),
        out_shape=(
            like(m), like(w_in), like(mom_in), like(mom_out), like(mom_out),
            like(grad_input), like(output), like(grad_in), like(grad_out),
        ),
        in_specs=[
            spec(cols, width), spec(8, cols), spec(8, width), spec(8, own_rows), into, into, out,
            whole, whole, part, part, into, out,
        ],
        out_specs=[spec(cols, width), into, into, out, out, part, part, into, out],
        compiler_params=params(),
        name="close",
    )(m, right, basis, mine, mom_in, w_in, mom_out, w_out, w_down, grad_input, output, grad_in, grad_out)


def on_device(
    activations, cotangent, doc_lengths, w_in, w_attn_out, w_down, gains, scale_param,
    mom_in, mom_out, mom_gain, mom_scale, error_buffer, factors,
):
    rows, width = activations.shape
    n = lax.axis_size("mp")
    data_par = lax.axis_size("dp")
    my_data = lax.axis_index("dp")
    count = rows * n
    scaling = (count * data_par) ** (-0.5)
    cols = w_in.shape[2]
    own_rows = w_in.shape[1]
    heads = cols // HD
    longest = count // 2
    span = min(n, -(-(longest - 1) // rows) + 1)
    dims = (n, rows, heads, span)

    ends = jnp.cumsum(doc_lengths[0])
    position = jnp.arange(count, dtype=jnp.int32)[:, None]
    starts = jnp.max(jnp.where(ends[None, :] <= position, ends[None, :], 0), axis=1, keepdims=True)
    factor = SCALE_BASE / math.sqrt(HD) * jax.nn.softplus(scale_param)
    c_row = jnp.tile(jnp.pad(factor, (0, LANE - HD)), heads)[None]

    n1, q, k, v, lse, oc, wqkv, w_tail, g_near, n2_near, output, dh, n2, dhb, dgain2 = front(
        dims, activations, cotangent, w_in, w_attn_out.T, w_down.T, gains, c_row, starts
    )
    wqkv, w_tail = wqkv.reshape(3, width, cols), w_tail.reshape(3, width, cols)
    dx, dc, dhb, g_mid = back(dims, q, k, v, lse, dhb, c_row, starts, w_tail, g_near)
    hbm = (n1, n2, n2_near, dhb, cotangent, g_near, g_mid, dx, oc, wqkv, w_tail, error_buffer[0])
    grad_in, out_sum, grad_input, basis, right, small, stored = grads(
        dims, scaling, hbm, activations, dh, gains, dgain2, dc, jnp.swapaxes(factors, 1, 2)
    )
    mine = lax.dynamic_slice_in_dim(basis, my_data * own_rows, own_rows, 2)
    error_new, new_in, mom_in_new, new_out, mom_out_new, grad_input, output, grad_in, grad_out = close(
        stored, right, basis, mine, mom_in, w_in, jnp.swapaxes(mom_out, 1, 2), w_attn_out.T, w_down.T,
        grad_input, output, grad_in, out_sum,
    )
    error_new = error_new[None]
    new_out, mom_out_new, grad_out = (jnp.swapaxes(x, 1, 2) for x in (new_out, mom_out_new, grad_out))
    tiles = width // LANE
    small = small.reshape(-1, LANE)
    grad_gain = small[: 2 * tiles].reshape(2, width)
    slope = (SCALE_BASE / math.sqrt(HD)) * jax.nn.sigmoid(scale_param) / factor
    grad_scale = small[2 * tiles, :HD] * slope
    right = jnp.swapaxes(right, 1, 2)
    mom_gain_new = MOMENTUM * mom_gain + grad_gain
    new_gain = gains - RATE * mom_gain_new
    mom_scale_new = MOMENTUM * mom_scale + grad_scale
    new_scale = scale_param - RATE * mom_scale_new
    return (
        output, grad_input, grad_in, grad_out, grad_gain, grad_scale, new_in, new_out,
        new_gain, new_scale, mom_in_new, mom_out_new, mom_gain_new, mom_scale_new,
        error_new, right,
    )


def solution(mesh):
    tokens, shard = P(("dp", "mp"), None), P(None, "dp", "mp")
    return jax.shard_map(
        on_device,
        mesh=mesh,
        in_specs=(
            tokens, tokens, P("dp", None), shard, P("mp", "dp"), P("mp", "dp"), P(), P(),
            shard, P(None, "mp", "dp"), P(), P(), P("dp", None, "mp", None), P(None, "mp", None),
        ),
        out_specs=(
            tokens, tokens, shard, P(None, "mp", "dp"), P(), P(), shard, P(None, "mp", "dp"),
            P(), P(), shard, P(None, "mp", "dp"), P(), P(), P("dp", None, "mp", None),
            P(None, "mp", None),
        ),
        check_vma=False,
    )
```
